256 devices in a mesh: replica: 16 (over z, core), seq: 4 (over x), tensor: 4 (over y).
Axes of the slice: x: 4, y: 4, z: 8, core: 2. Of those that a mesh axis runs over, the one named last changes fastest.
Arguments:
- residual: bfloat16 [16, 1024, 4096], P('replica'), may hold values from -15 to 15
- queries: bfloat16 [16, 1024, 4096], P('replica', 'seq', 'tensor'), may hold values from -40 to 40
- attn_keys: bfloat16 [16, 1024, 1024], P('replica', 'seq', 'tensor'), may hold values from -4 to 4
- attn_values: bfloat16 [16, 1024, 1024], P('replica', 'seq', 'tensor'), may hold values from -6 to 6
- lengths: int32 [16, 4], P('replica'), may hold values from 1 to 640, 1024 in all within a row
- requests: int32 [16, 4], P('replica'), may hold values from 1 to 256
- routes: int32 [16, 1024, 2], P('replica'), may hold values from 0 to 7, as said below
- out_weight: bfloat16 [4096, 4096], P('tensor', 'seq'), may hold values from -0.125 to 0.125
- norm_gain: float32 [4096], replicated, may hold values from 0.5 to 2
- router: bfloat16 [4096, 8], replicated, may hold values from -0.0234375 to 0.0234375
- w_gate: bfloat16 [1, 7168, 4096], P(None, ('seq', 'tensor')), may hold values from -0.09375 to 0.09375
- w_up: bfloat16 [1, 7168, 4096], P(None, ('seq', 'tensor')), may hold values from -0.09375 to 0.09375
- w_down: bfloat16 [1, 7168, 4096], P(None, ('seq', 'tensor')), may hold values from -0.09375 to 0.09375
Outputs:
- layer_out: bfloat16 [16, 1024, 4096], P('replica', 'seq', 'tensor')
The draws below stay inside these ranges and needn't reach their ends.
Inputs may be any that keep to these rules, and one draw needn't show every extreme that they name: Each replica's lengths sum to 1024. `routes`: the two experts of a slot differ.
All inputs are finite; a program needn't handle non-finite values.
Results may differ from the reference program's by a relative error of at most 0.01.
Values may be sent and summed in bfloat16 or wider, within the bound.
A program may use at most 128 MiB of HBM per device.

```python
import math
import jax
import jax.numpy as jnp
import numpy as np
from jax import lax

D = 4096
HEADS = 32
KV_HEADS = 8
HEAD_DIM = 128
EXPERTS = 8
FF_WIN = 7168
EXP_WIN = 1
TOK_DEV = 256
PROMPTS = 4
TOKENS = 1024
BLOCKS = 4
REPLICAS = 16
ALLOWANCE = 1024


def query_key_pair(key):
    base = jax.random.fold_in(key, 7)
    query_seed, key_seed = jax.random.split(base, 2)
    query_shape = (REPLICAS, TOKENS, HEADS * HEAD_DIM)
    key_shape = (REPLICAS, TOKENS, KV_HEADS * HEAD_DIM)
    keys_drawn = jnp.clip(jax.random.normal(key_seed, key_shape, jnp.float32), -4.0, 4.0)
    queries_drawn = jnp.clip(jax.random.normal(query_seed, query_shape, jnp.float32), -4.0, 4.0)
    return (queries_drawn, keys_drawn)


def draw_queries(key, part):
    return query_key_pair(key)[0].astype(jnp.bfloat16)


def draw_attn_keys(key, part):
    return query_key_pair(key)[1].astype(jnp.bfloat16)


def draw_residual(key, part):
    base_seed, row_seed, column_seed = jax.random.split(jax.random.fold_in(key, 3), 3)
    shape = (REPLICAS, TOKENS, D)
    base = jax.random.normal(base_seed, shape, jnp.float32)
    row_scale = jnp.exp(jax.random.uniform(row_seed, (REPLICAS, TOKENS, 1), jnp.float32, math.log(0.2), math.log(2.0)))
    column_scale = jnp.exp(jax.random.uniform(column_seed, (1, 1, D), jnp.float32, math.log(0.3), math.log(3.0)))
    return jnp.clip(base * row_scale * column_scale, -15.0, 15.0).astype(jnp.bfloat16)


def draw_requests(key, part):
    ranks = jnp.arange(REPLICAS, dtype=jnp.int32)[:, None]
    block_ids = jnp.arange(BLOCKS, dtype=jnp.int32)[None, :]
    percent = jnp.where(block_ids == 0, 45, jnp.where(block_ids == 1, 55, 65)).astype(jnp.int32)
    centre = TOK_DEV * percent * (REPLICAS - 1 + 2 * ranks) // (200 * (REPLICAS - 1))
    spread = max(TOK_DEV // 16, 1)
    jitter = jax.random.randint(jax.random.fold_in(key, 11), (REPLICAS, BLOCKS), -spread, spread + 1)
    drawn = jnp.clip(centre + jitter, 1, TOK_DEV)
    drawn = jnp.where((ranks == REPLICAS - 1) & (block_ids == 2), TOK_DEV, drawn)
    single = jax.random.randint(jax.random.fold_in(key, 13), (), 0, REPLICAS)
    drawn = jnp.where((ranks == single) & (block_ids == BLOCKS - 1), 1, drawn)
    return drawn.astype(jnp.int32)


def draw_routes(key, part):
    other_seed, pair_seed, side_seed, spot_seed = jax.random.split(jax.random.fold_in(key, 19), 4)
    shape = (REPLICAS, TOKENS)
    first = jax.random.randint(other_seed, shape, 1, EXPERTS)
    offset = jax.random.randint(pair_seed, shape, 1, EXPERTS - 1)
    second = (first - 1 + offset) % (EXPERTS - 1) + 1
    side = jax.random.randint(side_seed, shape, 0, 2)
    spot = jax.random.randint(spot_seed, (REPLICAS, TOKENS // TOK_DEV), 0, TOK_DEV)
    positions = jnp.arange(TOKENS, dtype=jnp.int32)
    excluded = (positions % TOK_DEV)[None, :] == jnp.repeat(spot, TOK_DEV, axis=1)
    leading = jnp.where(excluded, first, 0)
    trailing = jnp.where(excluded, second, first)
    column_one = jnp.where(side == 0, leading, trailing)
    column_two = jnp.where(side == 0, trailing, leading)
    return jnp.stack([column_one, column_two], axis=-1).astype(jnp.int32)


def strengthened(values, stream_key, source, target, shards_of, factor):
    owner, partner = [(jnp.arange(values.shape[dim]) // (values.shape[dim] // shards_of)).reshape([-1 if axis == dim else 1 for axis in range(values.ndim)]) for dim in (source, target)]
    chosen = jax.random.permutation(stream_key, shards_of)[partner]
    strong = (owner == chosen) | (owner == (partner + shards_of // 2) % shards_of)
    return jnp.where(strong, factor * values, values)


def steps_of(own_key, extent, cuts, least, largest):
    loudness = 1.0
    for axis_at, shards_of in cuts:
        heights = jax.random.uniform(jax.random.fold_in(jax.random.fold_in(own_key, 6), axis_at), (shards_of,), jnp.float32, least / len(cuts), largest / len(cuts))
        loudness = loudness * jnp.repeat(jnp.exp(heights), extent[axis_at] // shards_of).reshape((-1,) + (1,) * (len(extent) - 1 - axis_at))
    return loudness


def split_up(number_of, total, reach, slope):
    weights = [(1 << 20) // math.isqrt(grade ** slope) + 1 for grade in range(2, number_of + 1)]
    surplus, given = total - reach - (number_of - 1), [1] * (number_of - 1)
    while surplus > 0:
        free = [i for i in range(number_of - 1) if given[i] < reach]
        whole, remaining = sum([weights[i] for i in free]), surplus
        for i in free:
            addition = min(reach - given[i], max(1, remaining * weights[i] // whole), surplus)
            given[i] = given[i] + addition
            surplus = surplus - addition
    return np.array([reach] + given)


def ragged(key, count, total, reach, skew):
    if count == 2:
        one = jax.random.randint(key, (), max(1, total - reach), min(reach, total - 1) + 1)
        return jnp.stack([one, total - one])
    sizes = jnp.asarray(split_up(count, total, reach, skew), jnp.int32)
    twos = (count - 1) // 2
    donor, taker = sizes[1:1 + 2 * twos:2], sizes[2:2 + 2 * twos:2]
    room = jnp.minimum(donor - 1, reach - taker)
    moved = jax.random.randint(jax.random.fold_in(key, 1), (twos,), 0, 1 << 20) % (room + 1)
    sizes = sizes.at[1:1 + 2 * twos:2].set(donor - moved).at[2:2 + 2 * twos:2].set(taker + moved)
    return sizes[jax.random.permutation(jax.random.fold_in(key, 2), count)]


def gaussian(key, extent, deviation, most, pieces=(), kind=jnp.bfloat16):
    entries = deviation * jax.random.normal(key, extent, jnp.float32)
    if pieces:
        entries = entries * steps_of(key, extent, pieces, -0.22, 0.18)
    return jnp.clip(entries, -most, most).astype(kind)


def bell_draw_with(stream_key, shape, width, bound, cuts, heavy, held_as=jnp.bfloat16):
    entries = width * jax.random.normal(stream_key, shape, jnp.float32)
    if cuts:
        entries = entries * steps_of(stream_key, shape, cuts, -0.22, 0.18)
    return jnp.clip(strengthened(entries, jax.random.fold_in(stream_key, 3), *heavy), -bound, bound).astype(held_as)


def setup_inputs(seed: int = 0) -> dict:
    streams_of = jax.random.split(jax.random.key(seed), 14)
    return {
        "residual": draw_residual(jax.random.fold_in(streams_of[13], 71), 0),
        "queries": draw_queries(jax.random.fold_in(streams_of[13], 71), 0),
        "attn_keys": draw_attn_keys(jax.random.fold_in(streams_of[13], 71), 0),
        "attn_values": gaussian(streams_of[3], (REPLICAS, TOKENS, KV_HEADS * HEAD_DIM), 1.0, 6.0, ((0, 16), (1, 4), (2, 4))),
        "lengths": jax.vmap(lambda own: ragged(own, PROMPTS, TOKENS, TOKENS * 5 // 8, 2))(jax.random.split(streams_of[4], REPLICAS)).reshape((REPLICAS, PROMPTS)).astype(jnp.int32),
        "requests": draw_requests(jax.random.fold_in(streams_of[13], 71), 0),
        "routes": draw_routes(jax.random.fold_in(streams_of[13], 71), 0),
        "out_weight": bell_draw_with(streams_of[7], (HEADS * HEAD_DIM, D), (HEADS * HEAD_DIM) ** -0.5, 0.125, ((0, 4), (1, 4)), (0, 1, 4, 2.0)),
        "norm_gain": jnp.clip(jnp.exp(jax.random.uniform(streams_of[8], (D,), jnp.float32, math.log(0.5), math.log(2.0))), 0.5, 2.0),
        "router": gaussian(streams_of[9], (D, EXPERTS), (16 * D) ** -0.5, 0.0234375),
        "w_gate": gaussian(streams_of[10], (EXP_WIN, FF_WIN, D), D ** -0.5, 0.09375, ((1, 16),)),
        "w_up": gaussian(streams_of[11], (EXP_WIN, FF_WIN, D), D ** -0.5, 0.09375, ((1, 16),)),
        "w_down": bell_draw_with(streams_of[12], (EXP_WIN, FF_WIN, D), FF_WIN ** -0.5, 0.09375, ((1, 16),), (1, 2, 16, 2.0)),
    }


masked_score = -1e+30
epsilon = 1e-05

def admit(requests):
    columns = [requests[:, 0]]
    for block_index in range(1, BLOCKS):
        total = jnp.sum(columns[-1]).astype(jnp.int32)
        wanted = requests[:, block_index]
        columns.append(jnp.minimum(wanted, jnp.maximum(1, wanted * ALLOWANCE // total)).astype(jnp.int32))
    return jnp.stack(columns, axis=1)

def one_replica(residual, queries, attn_keys, attn_values, length_row, admitted_row, route_rows, out_weight, norm_gain, router, w_gate, w_up, w_down):
    positions = jnp.arange(TOKENS, dtype=jnp.int32)
    block_ids = jnp.arange(BLOCKS, dtype=jnp.int32)
    capacity = lax.optimization_barrier(jnp.sum(jnp.where((positions // TOK_DEV)[:, None] == block_ids[None, :], admitted_row[None, :], 0), axis=1)).astype(jnp.int32)
    live = positions % TOK_DEV < capacity
    ends = jnp.cumsum(length_row).astype(jnp.int32)
    begin = lax.optimization_barrier(jnp.sum(jnp.where(ends[None, :] <= positions[:, None], length_row[None, :], 0), axis=1)).astype(jnp.int32)
    allowed = (positions[None, :] <= positions[:, None]) & (positions[None, :] >= begin[:, None]) & (live[None, :] | (positions[None, :] == positions[:, None]))
    group = HEADS // KV_HEADS
    scale = 1.0 / math.sqrt(HEAD_DIM)
    query_heads = queries.reshape(TOKENS, HEADS, HEAD_DIM)
    key_heads = attn_keys.reshape(TOKENS, KV_HEADS, HEAD_DIM)
    value_heads = attn_values.reshape(TOKENS, KV_HEADS, HEAD_DIM)

    def per_head(head):
        source = head // group
        query_block = lax.dynamic_index_in_dim(query_heads, head, 1, keepdims=False)
        key_block = lax.dynamic_index_in_dim(key_heads, source, 1, keepdims=False)
        value_block = lax.dynamic_index_in_dim(value_heads, source, 1, keepdims=False)
        scores = jnp.dot(query_block, key_block.T, preferred_element_type=jnp.float32) * scale
        highest = lax.optimization_barrier(jnp.max(jnp.where(allowed, scores, masked_score), axis=1, keepdims=True))
        weights = jnp.where(allowed, jnp.exp(scores - highest), 0.0).astype(jnp.bfloat16)
        numer = jnp.dot(weights, value_block, preferred_element_type=jnp.float32)
        denom = lax.optimization_barrier(jnp.sum(weights.astype(jnp.float32), axis=1, keepdims=True))
        return (numer / denom).astype(jnp.bfloat16)
    heads_out = lax.map(per_head, jnp.arange(HEADS, dtype=jnp.int32))
    attended = jnp.transpose(heads_out, (1, 0, 2)).reshape(TOKENS, HEADS * HEAD_DIM)
    projected = jnp.dot(attended, out_weight, preferred_element_type=jnp.float32)
    stream = (residual.astype(jnp.float32) + projected).astype(jnp.bfloat16)
    wide = stream.astype(jnp.float32)
    normed = (wide * lax.rsqrt(lax.optimization_barrier(jnp.mean(wide * wide, axis=1, keepdims=True)) + epsilon) * norm_gain).astype(jnp.bfloat16)
    logits = jnp.dot(normed, router, preferred_element_type=jnp.float32)
    expert_ids = jnp.arange(EXPERTS, dtype=jnp.int32)
    first = lax.optimization_barrier(jnp.sum(jnp.where(route_rows[:, 0:1] == expert_ids[None, :], logits, 0.0), axis=1))
    second = lax.optimization_barrier(jnp.sum(jnp.where(route_rows[:, 1:2] == expert_ids[None, :], logits, 0.0), axis=1))
    weight_first = jax.nn.sigmoid(first - second)
    weight_second = jax.nn.sigmoid(second - first)
    mixed = jnp.zeros((TOKENS, D), jnp.float32)
    contract = (((1,), (1,)), ((), ()))
    for expert in range(EXP_WIN):
        combine = jnp.where(route_rows[:, 0] == expert, weight_first, 0.0) + jnp.where(route_rows[:, 1] == expert, weight_second, 0.0)
        gate = lax.dot_general(normed, w_gate[expert], contract, preferred_element_type=jnp.float32)
        upward = lax.dot_general(normed, w_up[expert], contract, preferred_element_type=jnp.float32)
        hidden = (jax.nn.silu(gate) * upward * combine[:, None]).astype(jnp.bfloat16)
        mixed = mixed + jnp.dot(hidden, w_down[expert], preferred_element_type=jnp.float32)
    return jnp.where(live[:, None], stream.astype(jnp.float32) + mixed, 0.0).astype(jnp.bfloat16)

def reference(residual, queries, attn_keys, attn_values, lengths, requests, routes, out_weight, norm_gain, router, w_gate, w_up, w_down):
    admitted = admit(requests)

    def step(item):
        return one_replica(item[0], item[1], item[2], item[3], item[4], item[5], item[6], out_weight, norm_gain, router, w_gate, w_up, w_down)
    return lax.map(step, (residual, queries, attn_keys, attn_values, lengths, admitted, routes))
```

```python
import functools
import math

import jax
import jax.numpy as jnp
from jax import lax
from jax.experimental import pallas as pl
from jax.experimental.pallas import tpu as pltpu
from jax.sharding import PartitionSpec as P

HEAD_DIM = 128
RING = 4
MESH = pl.DeviceIdType.MESH
VMEM = pltpu.VMEM
SIZES = (384, 640, 1024)

masked_score = -1e30
epsilon = 1e-05
f32 = jnp.float32
bf16 = jnp.bfloat16


class Copies:
    def __init__(self, send, recv):
        self.send, self.recv, self.count = send, recv, 0
        self.made = []

    def start(self, src, dst, where):
        n = self.count
        self.count += 1
        copy = pltpu.make_async_remote_copy(
            src_ref=src,
            dst_ref=dst,
            send_sem=self.send.at[n],
            recv_sem=self.recv.at[n],
            device_id=where,
            device_id_type=MESH,
        )
        copy.start()
        self.made.append(copy)
        return copy

    def drain(self):
        for copy in self.made:
            copy.wait_send()


class Ring:
    def __init__(self, axis):
        self.axis = axis
        self.me = lax.axis_index(axis)
        self.next = {axis: self.at(1)}
        self.prev = {axis: self.at(RING - 1)}

    def at(self, step):
        return lax.rem(self.me + step, RING)


def greet(devices):
    barrier = pltpu.get_barrier_semaphore()
    for device in devices:
        pl.semaphore_signal(barrier, inc=1, device_id=device, device_id_type=MESH)
    pl.semaphore_wait(barrier, len(devices))


def span(index, size):
    return pl.ds(pl.multiple_of(index * size, size), size)


class RingSum:
    def __init__(self, copies, ring, block, slots):
        self.copies, self.ring, self.block, self.slots = copies, ring, block, slots

    def raw(self):
        c, r, s = self.copies, self.ring, self.slots
        self.a = c.start(self.block(r.at(2), 0), s.at[0], r.next)
        self.b = c.start(self.block(r.at(2), 1), s.at[1], r.prev)
        self.c = c.start(self.block(r.at(1), 1), s.at[2], r.next)
        self.d = c.start(self.block(r.at(3), 0), s.at[3], r.prev)

    def middle(self):
        c, r, s = self.copies, self.ring, self.slots
        self.a.wait_recv()
        s[6] = (self.block(r.at(1), 0)[...].astype(f32) + s[0].astype(f32)).astype(bf16)
        self.e = c.start(s.at[6], s.at[4], r.next)
        self.b.wait_recv()
        s[7] = (self.block(r.at(3), 1)[...].astype(f32) + s[1].astype(f32)).astype(bf16)
        self.f = c.start(s.at[7], s.at[5], r.prev)

    def total(self, half):
        s = self.slots
        if half == 0:
            self.d.wait_recv()
            self.e.wait_recv()
            near, far = s[3], s[4]
        else:
            self.c.wait_recv()
            self.f.wait_recv()
            near, far = s[2], s[5]
        own = self.block(self.ring.me, half)[...]
        return own.astype(f32) + near.astype(f32) + far.astype(f32)


def attention_kernel(
    replicas, req_ref, len_ref, q_ref, k_ref, v_ref,
    att_ref, col_ref, lane_ref, most_ref,
    every, kv, bias, send, recv, req_send, req_recv,
):
    seq = Ring("seq")
    me = lax.axis_index("replica")
    rows = q_ref.shape[0]
    slots = RING * rows
    wide = k_ref.shape[1]
    kv_count = wide // HEAD_DIM
    group = q_ref.shape[1] // wide
    others = [{"replica": lax.rem(me + d, replicas)} for d in range(1, replicas)]
    greet([seq.next, seq.prev] + others)
    asked = Copies(req_send, req_recv)
    for other in others:
        asked.start(req_ref, every.at[me], other)
    c = Copies(send, recv)
    own_k, own_v = kv.at[seq.me, :, pl.ds(0, wide)], kv.at[seq.me, :, pl.ds(wide, wide)]
    first = [
        c.start(ref, place, where)
        for where in (seq.next, seq.prev)
        for ref, place in ((k_ref, own_k), (v_ref, own_v))
    ]
    kv[seq.me, :, pl.ds(0, wide)] = k_ref[...]
    kv[seq.me, :, pl.ds(wide, wide)] = v_ref[...]
    every[me] = req_ref[...]

    for copy in asked.made:
        copy.wait_recv()
    wanted = jnp.max(every[...], axis=1)
    lane = lax.broadcasted_iota(jnp.int32, wanted.shape, 1)
    admitted = jnp.where(lane == 0, wanted, 0.0)
    for b in range(1, RING):
        total = jnp.sum(
            jnp.sum(jnp.where(lane == b - 1, admitted, 0.0), axis=1, keepdims=True), axis=0, keepdims=True
        )
        scaled = wanted * float(replicas * rows // 4)
        share = jnp.floor(scaled / total)
        left = scaled - share * total
        share = jnp.where(left < 0, share - 1, jnp.where(left >= total, share + 1, share))
        admitted = jnp.where(lane == b, jnp.minimum(wanted, jnp.maximum(1.0, share)), admitted)
    most = jnp.max(jnp.sum(admitted, axis=1, keepdims=True), axis=0, keepdims=True)
    most_ref[...] = jnp.broadcast_to(most, most_ref.shape).astype(jnp.int32)
    mine = lax.broadcasted_iota(jnp.int32, wanted.shape, 0) == me
    row = jnp.sum(jnp.where(mine, admitted, 0.0), axis=0, keepdims=True)
    lane_one = lax.broadcasted_iota(jnp.int32, row.shape, 1)
    caps = [jnp.sum(jnp.where(lane_one == b, row, 0.0), axis=1, keepdims=True).astype(jnp.int32) for b in range(RING)]
    length = jnp.max(len_ref[...], axis=0, keepdims=True)
    lens = [jnp.sum(jnp.where(lane_one == b, length, 0.0), axis=1, keepdims=True).astype(jnp.int32) for b in range(RING)]

    def slot_of(place):
        found = jnp.full(place.shape, -1, jnp.int32)
        start = jnp.zeros((1, 1), jnp.int32)
        for b in range(RING):
            stop = start + caps[b]
            found = jnp.where((place >= start) & (place < stop), place - start + b * rows, found)
            start = stop
        return found

    col_ref[...] = slot_of(lax.broadcasted_iota(jnp.int32, col_ref.shape, 0))
    lane_ref[...] = slot_of(lax.broadcasted_iota(jnp.int32, lane_ref.shape, 1))

    key = lax.broadcasted_iota(jnp.int32, (1, slots), 1)
    live = jnp.zeros((1, slots), jnp.int32)
    for b in range(RING):
        live = jnp.where((key >= b * rows) & (key < b * rows + caps[b]), 1, live)
    query = lax.broadcasted_iota(jnp.int32, (rows, 1), 0) + seq.me * rows
    begin = jnp.zeros((rows, 1), jnp.int32)
    end = jnp.zeros((1, 1), jnp.int32)
    for j in range(RING):
        end = end + lens[j]
        begin = begin + jnp.where(end <= query, lens[j], 0)
    allowed = (key <= query) & (key >= begin) & ((live == 1) | (key == query))
    bias[...] = jnp.where(allowed, 0.0, masked_score)

    half = rows // 2
    first[0].wait_recv()
    first[1].wait_recv()
    before, after = kv.at[seq.at(3), pl.ds(0, half)], kv.at[seq.at(1), pl.ds(half, half)]
    on = c.start(before, before, seq.next)
    first[2].wait_recv()
    first[3].wait_recv()
    back = c.start(after, after, seq.prev)
    on.wait_recv()
    back.wait_recv()

    scale = 1.0 / math.sqrt(HEAD_DIM)
    span_g = group * HEAD_DIM
    sent = []
    for g in range(kv_count):
        keys = kv[:, :, g * HEAD_DIM:(g + 1) * HEAD_DIM].reshape(slots, HEAD_DIM)
        values = kv[:, :, wide + g * HEAD_DIM:wide + (g + 1) * HEAD_DIM].reshape(slots, HEAD_DIM)

        @pl.loop(0, group)
        def _(h):
            cols = span(h + g * group, HEAD_DIM)
            scores = lax.dot_general(
                q_ref[:, cols], keys, (((1,), (1,)), ((), ())), preferred_element_type=f32
            ) * scale + bias[...]
            highest = jnp.max(scores, axis=1, keepdims=True)
            weights = jnp.exp(scores - highest).astype(bf16)
            norm = jnp.sum(weights.astype(f32), axis=1, keepdims=True)
            out = jnp.dot(weights, values, preferred_element_type=f32)
            att_ref[span(seq.me, rows), cols] = (out / norm).astype(bf16)

        mine = att_ref.at[span(seq.me, rows), pl.ds(g * span_g, span_g)]
        sent.append((c.start(mine, mine, seq.next), c.start(mine, mine, seq.prev)))
    passed = []
    part = span_g // 2
    for g in range(kv_count):
        sent[g][0].wait_recv()
        there = att_ref.at[span(seq.at(3), rows), pl.ds(g * span_g, part)]
        passed.append(c.start(there, there, seq.next))
        sent[g][1].wait_recv()
        there = att_ref.at[span(seq.at(1), rows), pl.ds(g * span_g + part, part)]
        passed.append(c.start(there, there, seq.prev))
    for copy in passed:
        copy.wait_recv()
    asked.drain()
    c.drain()


def attend(replicas, requests, lengths, queries, keys, values):
    rows, cols = queries.shape
    slots = RING * rows
    groups = keys.shape[1] // HEAD_DIM
    count = 4 + 2 + 4 * groups
    vmem = pl.BlockSpec(memory_space=VMEM)
    return pl.pallas_call(
        functools.partial(attention_kernel, replicas),
        out_shape=(
            jax.ShapeDtypeStruct((slots, cols), bf16),
            jax.ShapeDtypeStruct((slots, 128), jnp.int32),
            jax.ShapeDtypeStruct((8, slots), jnp.int32),
            jax.ShapeDtypeStruct((8, 128), jnp.int32),
        ),
        in_specs=[vmem] * 5,
        out_specs=(vmem,) * 4,
        scratch_shapes=[
            VMEM((replicas, 8, 128), f32),
            VMEM((RING, rows, 2 * keys.shape[1]), bf16),
            VMEM((rows, slots), f32),
            pltpu.SemaphoreType.DMA((count,)),
            pltpu.SemaphoreType.DMA((count,)),
            pltpu.SemaphoreType.DMA((replicas - 1,)),
            pltpu.SemaphoreType.DMA((replicas - 1,)),
        ],
        compiler_params=pltpu.CompilerParams(
            collective_id=0, has_side_effects=True, vmem_limit_bytes=40 << 20
        ),
        name="attend",
    )(requests, lengths, queries, keys, values)


def stream_kernel(part_ref, res_ref, out_ref, slots, send, recv):
    seq, ten = Ring("seq"), Ring("tensor")
    rows, cols = res_ref.shape
    half, quarter = cols // 2, cols // 4
    greet([seq.next, seq.prev, ten.next, ten.prev])
    c = Copies(send, recv)
    summed = RingSum(
        c, ten, lambda b, h: part_ref.at[span(b, rows), pl.ds(h * half, half)], slots
    )
    summed.raw()
    summed.middle()

    def tile(t, s, h, q=None):
        if q is None:
            return out_ref.at[span(t, rows), pl.ds(pl.multiple_of(s * cols + h * half, half), half)]
        return out_ref.at[
            span(t, rows), pl.ds(pl.multiple_of(s * cols + h * half + q * quarter, quarter), quarter)
        ]

    def both(ref, ring):
        return c.start(ref, ref, ring.next), c.start(ref, ref, ring.prev)

    def hop(ref, where):
        return c.start(ref, ref, where)

    def place(h, first, second):
        return (first, second) if h == 1 else (second, first)

    near, wide_sends = {}, {}
    for h, ring in ((0, seq), (1, ten)):
        tile(ten.me, seq.me, h)[...] = (
            res_ref[:, h * half:(h + 1) * half].astype(f32) + summed.total(h)
        ).astype(bf16)
        near[h] = both(tile(ten.me, seq.me, h), ring)
    for h, other in ((0, ten), (1, seq)):
        wide_sends[h] = [both(tile(ten.me, seq.me, h), other)]

    def where_of(h, step):
        return (ten.me, seq.at(step)) if h == 0 else (ten.at(step), seq.me)

    far = {}
    for h, ring in ((0, seq), (1, ten)):
        near[h][0].wait_recv()
        t, s = where_of(h, 3)
        far[h] = [hop(tile(t, s, h, 0), ring.next)]
        near[h][1].wait_recv()
        t, s = where_of(h, 1)
        far[h].append(hop(tile(t, s, h, 1), ring.prev))
    for step in (3, 1):
        for h, other in ((0, ten), (1, seq)):
            t, s = where_of(h, step)
            wide_sends[h].append(both(tile(t, s, h), other))
    for h, other in ((0, ten), (1, seq)):
        far[h][0].wait_recv()
        far[h][1].wait_recv()
        t, s = where_of(h, 2)
        wide_sends[h].append(both(tile(t, s, h), other))
    last = []
    for i, step in enumerate((0, 3, 1, 2)):
        for h, other in ((0, ten), (1, seq)):
            t, s = where_of(h, step)

            def across(k):
                return (other.at(k), s) if h == 0 else (t, other.at(k))

            wide_sends[h][i][0].wait_recv()
            last.append(hop(tile(*across(3), h, 0), other.next))
            wide_sends[h][i][1].wait_recv()
            last.append(hop(tile(*across(1), h, 1), other.prev))
    for copy in last:
        copy.wait_recv()
    c.drain()


def gather_stream(partial_value, residual, collective_id):
    rows, cols = residual.shape
    vmem = pl.BlockSpec(memory_space=VMEM)
    count = 6 + 2 * (4 + 8 + 8)
    return pl.pallas_call(
        stream_kernel,
        out_shape=jax.ShapeDtypeStruct((RING * rows, RING * cols), bf16),
        in_specs=[vmem] * 2,
        out_specs=vmem,
        scratch_shapes=[
            VMEM((8, rows, cols // 2), bf16),
            pltpu.SemaphoreType.DMA((count,)),
            pltpu.SemaphoreType.DMA((count,)),
        ],
        compiler_params=pltpu.CompilerParams(
            collective_id=collective_id, has_side_effects=True, vmem_limit_bytes=40 << 20
        ),
        name="stream",
    )(partial_value, residual)


def mix_kernel(part_ref, own_ref, out_ref, slots, sums, late, send, recv):
    seq, ten = Ring("seq"), Ring("tensor")
    rows, cols = own_ref.shape
    half, quarter, eighth = cols // 2, cols // 4, cols // 8
    greet([seq.next, seq.prev, ten.next, ten.prev])
    c = Copies(send, recv)
    order = (2, 1, 3, 0)

    def term(row, col, h, q):
        return part_ref.at[
            span(row, rows), pl.ds(pl.multiple_of(col * cols + h * half + q * quarter, quarter), quarter)
        ]

    early = {0: [], 1: []}
    for i, step in enumerate(order):
        row, col = seq.at(step), ten.at(step)
        early[0].append(
            RingSum(c, ten, lambda b, q, row=row: term(row, b, 0, q), slots.at[0, i])
        )
        early[1].append(
            RingSum(c, seq, lambda b, q, col=col: term(b, col, 1, q), slots.at[1, i])
        )

    def raw(i):
        early[0][i].raw()
        early[1][i].raw()

    def middle(i):
        early[0][i].middle()
        early[1][i].middle()

    def finish(i):
        for h, ring in ((0, seq), (1, ten)):
            for q in range(2):
                sums[h, ring.at(order[i]), :, q * quarter:(q + 1) * quarter] = (
                    early[h][i].total(q).astype(bf16)
                )

    raw(0)
    raw(1)
    for i in range(RING):
        middle(i)
        if i + 2 < RING:
            raw(i + 2)
    for i in range(RING):
        finish(i)
    final = [
        RingSum(
            c,
            ring,
            lambda b, q, h=h: sums.at[h, b, :, pl.ds(q * quarter, quarter)],
            late.at[h],
        )
        for h, ring in ((0, seq), (1, ten))
    ]
    for f in final:
        f.raw()
    for f in final:
        f.middle()
    sent = []
    for h in range(2):
        for q in range(2):
            at = h * half + q * quarter
            mine = out_ref.at[span(seq.me, rows), pl.ds(at, quarter)]
            mine[...] = (
                own_ref[:, at:at + quarter].astype(f32) + final[h].total(q)
            ).astype(bf16)
            sent.append((c.start(mine, mine, seq.next), c.start(mine, mine, seq.prev)))
    passed = []
    for k in range(4):
        at = k * quarter
        sent[k][0].wait_recv()
        there = out_ref.at[span(seq.at(3), rows), pl.ds(at, eighth)]
        passed.append(c.start(there, there, seq.next))
        sent[k][1].wait_recv()
        there = out_ref.at[span(seq.at(1), rows), pl.ds(at + eighth, eighth)]
        passed.append(c.start(there, there, seq.prev))
    for copy in passed:
        copy.wait_recv()
    c.drain()


def gather_mixed(partial_out, own_stream, collective_id):
    rows, cols = own_stream.shape
    vmem = pl.BlockSpec(memory_space=VMEM)
    count = 10 * 6 + 16
    return pl.pallas_call(
        mix_kernel,
        out_shape=jax.ShapeDtypeStruct((RING * rows, cols), bf16),
        in_specs=[vmem] * 2,
        out_specs=vmem,
        scratch_shapes=[
            VMEM((2, RING, 8, rows, cols // 4), bf16),
            VMEM((2, RING, rows, cols // 2), bf16),
            VMEM((2, 8, rows, cols // 4), bf16),
            pltpu.SemaphoreType.DMA((count,)),
            pltpu.SemaphoreType.DMA((count,)),
        ],
        compiler_params=pltpu.CompilerParams(
            collective_id=collective_id, has_side_effects=True, vmem_limit_bytes=50 << 20
        ),
        name="mix",
    )(partial_out, own_stream)


def dot(a, b, contract):
    return lax.dot_general(a, b, (contract, ((), ())), preferred_element_type=f32)


def packed_layer(
    size, index, attended, slot_col, slot_lane, residual, routes, out_weight, norm_gain, router, w_gate, w_up, w_down
):
    slots = attended.shape[0]
    rows_dev = slots // RING
    piece = size // RING
    seq_index = lax.axis_index("seq")
    tensor_index = lax.axis_index("tensor")
    positions = jnp.arange(slots, dtype=jnp.int32)
    width = out_weight.shape[1]
    pick = (slot_col[:size] == positions[None, :]).astype(bf16)
    packed = dot(pick, attended, ((1,), (0,))).astype(bf16)
    partial_value = dot(packed, out_weight, ((1,), (0,))).astype(bf16)
    own_pick = lax.dynamic_slice(slot_col, (tensor_index * piece, 0), (piece, 1))
    own_res = dot(
        (own_pick == positions[None, :]).astype(bf16),
        lax.dynamic_slice(residual, (0, seq_index * width), (slots, width)),
        ((1,), (0,)),
    ).astype(bf16)
    stream = gather_stream(partial_value, own_res, 1 + 2 * index)
    wide = stream.astype(f32)
    normed = (
        wide * lax.rsqrt(jnp.mean(wide * wide, axis=1, keepdims=True) + epsilon) * norm_gain
    ).astype(bf16)
    chosen = dot(pick, routes.astype(bf16), ((1,), (0,))).astype(jnp.int32)
    logits = dot(normed, router, ((1,), (0,)))
    expert_ids = jnp.arange(router.shape[1], dtype=jnp.int32)
    first = jnp.sum(jnp.where(chosen[:, 0:1] == expert_ids[None, :], logits, 0.0), axis=1, keepdims=True)
    second = jnp.sum(jnp.where(chosen[:, 1:2] == expert_ids[None, :], logits, 0.0), axis=1, keepdims=True)
    weight_first = jax.nn.sigmoid(first - second)
    weight_second = jax.nn.sigmoid(second - first)
    partial_out = None
    for e in range(w_gate.shape[0]):
        combine = jnp.where(chosen[:, 0:1] == e, weight_first, 0.0) + jnp.where(
            chosen[:, 1:2] == e, weight_second, 0.0
        )
        gate = dot(normed, w_gate[e], ((1,), (1,)))
        upward = dot(normed, w_up[e], ((1,), (1,)))
        hidden = (jax.nn.silu(gate) * upward * combine).astype(bf16)
        down = dot(hidden, w_down[e], ((1,), (0,)))
        partial_out = down if partial_out is None else partial_out + down
    own_stream = lax.dynamic_slice(stream, (seq_index * piece, tensor_index * width), (piece, width))
    packed_out = gather_mixed(partial_out.astype(bf16), own_stream, 2 + 2 * index)
    query_pos = seq_index * rows_dev + jnp.arange(rows_dev, dtype=jnp.int32)
    spread = (query_pos[:, None] == slot_lane[:1, :size]).astype(bf16)
    return dot(spread, packed_out, ((1,), (0,))).astype(bf16)


def shards(
    residual, queries, attn_keys, attn_values, lengths, requests, routes,
    out_weight, norm_gain, router, w_gate, w_up, w_down,
):
    replicas = lax.axis_size("replica")

    def widened(row):
        return jnp.broadcast_to(jnp.pad(row.astype(f32), ((0, 0), (0, 128 - row.shape[1]))), (8, 128))

    attended, slot_col, slot_lane, most = attend(
        replicas, widened(requests), widened(lengths), queries[0], attn_keys[0], attn_values[0]
    )
    slots = attended.shape[0]
    sizes = [n for n in SIZES if n < slots] + [slots]
    choice = jnp.sum(most[0, 0] > jnp.array(sizes[:-1], jnp.int32)).astype(jnp.int32)
    out = lax.switch(
        choice,
        [functools.partial(packed_layer, n, i) for i, n in enumerate(sizes)],
        attended, slot_col[:, :1], slot_lane, residual[0], routes[0],
        out_weight, norm_gain, router, w_gate, w_up, w_down,
    )
    return out[None]


def solution(mesh):
    return jax.shard_map(
        shards,
        mesh=mesh,
        in_specs=(
            P("replica", None, None),
            P("replica", "seq", "tensor"),
            P("replica", "seq", "tensor"),
            P("replica", "seq", "tensor"),
            P("replica", None),
            P("replica", None),
            P("replica", None, None),
            P("tensor", "seq"),
            P(),
            P(),
            P(None, ("seq", "tensor"), None),
            P(None, ("seq", "tensor"), None),
            P(None, ("seq", "tensor"), None),
        ),
        out_specs=P("replica", "seq", "tensor"),
        check_vma=False,
    )
```

```python
import functools
import math

import jax
import jax.numpy as jnp
from jax import lax
from jax.experimental import pallas as pl
from jax.experimental.pallas import tpu as pltpu
from jax.sharding import PartitionSpec as P

HEAD_DIM = 128
RING = 4
MESH = pl.DeviceIdType.MESH
VMEM = pltpu.VMEM
WINDOW = 640

masked_score = -1e30
epsilon = 1e-05
f32 = jnp.float32
bf16 = jnp.bfloat16


class Copies:
    def __init__(self, send, recv):
        self.send, self.recv, self.count = send, recv, 0
        self.made = []

    def start(self, src, dst, where):
        n = self.count
        self.count += 1
        copy = pltpu.make_async_remote_copy(
            src_ref=src,
            dst_ref=dst,
            send_sem=self.send.at[n],
            recv_sem=self.recv.at[n],
            device_id=where,
            device_id_type=MESH,
        )
        copy.start()
        self.made.append(copy)
        return copy

    def drain(self):
        for copy in self.made:
            copy.wait_send()


class Ring:
    def __init__(self, axis):
        self.axis = axis
        self.me = lax.axis_index(axis)
        self.next = {axis: self.at(1)}
        self.prev = {axis: self.at(RING - 1)}

    def at(self, step):
        return lax.rem(self.me + step, RING)


def greet(devices):
    barrier = pltpu.get_barrier_semaphore()
    for device in devices:
        pl.semaphore_signal(barrier, inc=1, device_id=device, device_id_type=MESH)
    pl.semaphore_wait(barrier, len(devices))


def span(index, size):
    return pl.ds(pl.multiple_of(index * size, size), size)


def dot(a, b, contract):
    return lax.dot_general(a, b, (contract, ((), ())), preferred_element_type=f32)


PLAIN = ((1,), (0,))
TURNED = ((1,), (1,))


class RingSum:
    def __init__(self, copies, ring, block, slots):
        self.copies, self.ring, self.block, self.slots = copies, ring, block, slots

    def far(self):
        c, r, s = self.copies, self.ring, self.slots
        self.a = c.start(self.block(2, 0), s.at[0], r.next)
        self.b = c.start(self.block(2, 1), s.at[1], r.prev)

    def ahead(self):
        self.c = self.copies.start(self.block(1, 1), self.slots.at[2], self.ring.next)

    def behind(self):
        self.d = self.copies.start(self.block(3, 0), self.slots.at[3], self.ring.prev)

    def raw(self):
        self.far()
        self.ahead()
        self.behind()

    def middle(self):
        c, r, s = self.copies, self.ring, self.slots
        self.a.wait_recv()
        s[6] = (self.block(1, 0)[...].astype(f32) + s[0].astype(f32)).astype(bf16)
        self.e = c.start(s.at[6], s.at[4], r.next)
        self.b.wait_recv()
        s[7] = (self.block(3, 1)[...].astype(f32) + s[1].astype(f32)).astype(bf16)
        self.f = c.start(s.at[7], s.at[5], r.prev)

    def total(self, half):
        s = self.slots
        if half == 0:
            self.d.wait_recv()
            self.e.wait_recv()
            near, far = s[3], s[4]
        else:
            self.c.wait_recv()
            self.f.wait_recv()
            near, far = s[2], s[5]
        own = self.block(0, half)[...]
        return own.astype(f32) + near.astype(f32) + far.astype(f32)


def attention_kernel(
    replicas, req_ref, len_ref, routes_ref, q_hbm, k_hbm, v_hbm, w_hbm, res_hbm,
    part_ref, own_ref, delta_ref, lane_ref, most_ref,
    req, every, q_ref, kv, bias, pick, att_ref, w_ref, res_ref, proj,
    local, send, recv, req_send, req_recv,
):
    seq = Ring("seq")
    me = lax.axis_index("replica")
    rows = q_ref.shape[0]
    slots = RING * rows
    wide = k_hbm.shape[1]
    kv_count = wide // HEAD_DIM
    group = q_ref.shape[1] // wide
    cols = w_ref.shape[1]
    loads = [
        pltpu.make_async_copy(src, dst, local.at[i])
        for i, (src, dst) in enumerate((
            (k_hbm, kv.at[seq.me, :, pl.ds(0, wide)]),
            (v_hbm, kv.at[seq.me, :, pl.ds(wide, wide)]),
            (q_hbm, q_ref),
            (res_hbm.at[:, span(seq.me, cols)], res_ref),
            (w_hbm, w_ref),
        ))
    ]
    for load in loads:
        load.start()
    req[...] = jnp.zeros_like(req)
    req[0:1, 0:RING] = req_ref[...].astype(f32)
    others = [{"replica": lax.rem(me + d, replicas)} for d in range(1, replicas)]
    greet([seq.next, seq.prev] + others)
    c = Copies(send, recv)
    loads[0].wait()
    loads[1].wait()
    first = [c.start(kv.at[seq.me], kv.at[seq.me], where) for where in (seq.next, seq.prev)]
    asked = Copies(req_send, req_recv)
    for other in others:
        asked.start(req, every.at[me], other)
    every[me] = req[...]

    for copy in asked.made:
        copy.wait_recv()
    wanted = jnp.max(every[...], axis=1)
    lane = lax.broadcasted_iota(jnp.int32, wanted.shape, 1)
    admitted = jnp.where(lane == 0, wanted, 0.0)
    for b in range(1, RING):
        total = jnp.sum(
            jnp.sum(jnp.where(lane == b - 1, admitted, 0.0), axis=1, keepdims=True), axis=0, keepdims=True
        )
        scaled = wanted * float(replicas * rows // 4)
        share = jnp.floor(scaled / total)
        left = scaled - share * total
        share = jnp.where(left < 0, share - 1, jnp.where(left >= total, share + 1, share))
        admitted = jnp.where(lane == b, jnp.minimum(wanted, jnp.maximum(1.0, share)), admitted)
    most = jnp.max(jnp.sum(admitted, axis=1, keepdims=True), axis=0, keepdims=True)
    most_ref[...] = jnp.broadcast_to(most, most_ref.shape).astype(jnp.int32)
    mine = lax.broadcasted_iota(jnp.int32, wanted.shape, 0) == me
    row = jnp.sum(jnp.where(mine, admitted, 0.0), axis=0, keepdims=True)
    lane_one = lax.broadcasted_iota(jnp.int32, row.shape, 1)
    caps = [jnp.sum(jnp.where(lane_one == b, row, 0.0), axis=1, keepdims=True).astype(jnp.int32) for b in range(RING)]
    prompts = len_ref.shape[1]
    length = len_ref[...].astype(f32)
    lane_len = lax.broadcasted_iota(jnp.int32, length.shape, 1)
    lens = [
        jnp.sum(jnp.where(lane_len == b, length, 0.0), axis=1, keepdims=True).astype(jnp.int32)
        for b in range(prompts)
    ]

    def slot_of(place):
        found = jnp.full(place.shape, -1, jnp.int32)
        start = jnp.zeros((1, 1), jnp.int32)
        for b in range(RING):
            stop = start + caps[b]
            found = jnp.where((place >= start) & (place < stop), place - start + b * rows, found)
            start = stop
        return found

    lane_ref[...] = slot_of(lax.broadcasted_iota(jnp.int32, lane_ref.shape, 1))
    key = lax.broadcasted_iota(jnp.int32, (1, slots), 1)
    live = jnp.zeros((1, slots), jnp.int32)
    for b in range(RING):
        live = jnp.where((key >= b * rows) & (key < b * rows + caps[b]), 1, live)
    query = lax.broadcasted_iota(jnp.int32, (rows, 1), 0) + seq.me * rows
    begin = jnp.zeros((rows, 1), jnp.int32)
    end = jnp.zeros((1, 1), jnp.int32)
    for j in range(prompts):
        end = end + lens[j]
        begin = begin + jnp.where(end <= query, lens[j], 0)
    allowed = (key <= query) & (key >= begin) & ((live == 1) | (key == query))
    bias[...] = jnp.where(allowed, 0.0, masked_score)

    half = rows // 2
    first[0].wait_recv()
    before, after = kv.at[seq.at(3), pl.ds(0, half)], kv.at[seq.at(1), pl.ds(half, half)]
    on = c.start(before, before, seq.next)
    first[1].wait_recv()
    back = c.start(after, after, seq.prev)

    @pl.loop(0, slots // 128)
    def _(i):
        place = lax.broadcasted_iota(jnp.int32, (128, 1), 0) + i * 128
        pick[span(i, 128), :] = jnp.where(slot_of(place) == key, 1.0, 0.0).astype(bf16)

    expert = lax.broadcasted_iota(jnp.int32, (128, slots), 0)
    gap = jnp.where(routes_ref[0:1, :] == expert, 1.0, 0.0) - jnp.where(routes_ref[1:2, :] == expert, 1.0, 0.0)
    delta_ref[...] = dot(pick[...], gap.astype(bf16), TURNED)
    on.wait_recv()
    back.wait_recv()
    loads[2].wait()

    scale = 1.0 / math.sqrt(HEAD_DIM)
    span_g = group * HEAD_DIM
    sent = []
    for g in range(kv_count):
        keys = kv[:, :, g * HEAD_DIM:(g + 1) * HEAD_DIM].reshape(slots, HEAD_DIM)
        values = kv[:, :, wide + g * HEAD_DIM:wide + (g + 1) * HEAD_DIM].reshape(slots, HEAD_DIM)

        @pl.loop(0, group)
        def _(h):
            at = span(h + g * group, HEAD_DIM)
            scores = dot(q_ref[:, at], keys, TURNED) * scale + bias[...]
            highest = jnp.max(scores, axis=1, keepdims=True)
            weights = jnp.exp(scores - highest).astype(bf16)
            norm = jnp.sum(weights.astype(f32), axis=1, keepdims=True)
            att_ref[span(seq.me, rows), at] = (dot(weights, values, PLAIN) / norm).astype(bf16)

        mine = att_ref.at[span(seq.me, rows), pl.ds(g * span_g, span_g)]
        sent.append((c.start(mine, mine, seq.next), c.start(mine, mine, seq.prev)))

    def project(block, start):
        proj[...] = dot(att_ref[span(block, rows), :], w_ref[...], PLAIN).astype(bf16)

        @pl.loop(0, RING)
        def _(i):
            chosen = dot(pick[span(i, rows), span(block, rows)], proj[...], PLAIN)
            if not start:
                chosen = chosen + part_ref[span(i, rows), :].astype(f32)
            part_ref[span(i, rows), :] = chosen.astype(bf16)

    loads[3].wait()

    @pl.loop(0, RING)
    def _(i):
        own_ref[span(i, rows), :] = dot(pick[span(i, rows), :], res_ref[...], PLAIN).astype(bf16)

    loads[4].wait()
    project(seq.me, True)
    passed = []
    part = span_g // 2
    for g in range(kv_count):
        sent[g][0].wait_recv()
        there = att_ref.at[span(seq.at(3), rows), pl.ds(g * span_g, part)]
        passed.append(c.start(there, there, seq.next))
        sent[g][1].wait_recv()
        there = att_ref.at[span(seq.at(1), rows), pl.ds(g * span_g + part, part)]
        passed.append(c.start(there, there, seq.prev))
    project(seq.at(3), False)
    project(seq.at(1), False)
    for copy in passed:
        copy.wait_recv()
    project(seq.at(2), False)
    asked.drain()
    c.drain()


def attend(replicas, requests, lengths, routes, queries, keys, values, out_weight, residual):
    rows, heads = queries.shape
    slots = RING * rows
    cols = out_weight.shape[1]
    groups = keys.shape[1] // HEAD_DIM
    count = 4 + 4 * groups
    vmem = pl.BlockSpec(memory_space=VMEM)
    hbm = pl.BlockSpec(memory_space=pltpu.HBM)
    dma = pltpu.SemaphoreType.DMA
    return pl.pallas_call(
        functools.partial(attention_kernel, replicas),
        out_shape=(
            jax.ShapeDtypeStruct((slots, cols), bf16),
            jax.ShapeDtypeStruct((slots, cols), bf16),
            jax.ShapeDtypeStruct((slots, 128), f32),
            jax.ShapeDtypeStruct((8, slots), jnp.int32),
            jax.ShapeDtypeStruct((8, 128), jnp.int32),
        ),
        in_specs=[vmem] * 3 + [hbm] * 5,
        out_specs=(vmem,) * 5,
        scratch_shapes=[
            VMEM((8, 128), f32),
            VMEM((replicas, 8, 128), f32),
            VMEM((rows, heads), bf16),
            VMEM((RING, rows, 2 * keys.shape[1]), bf16),
            VMEM((rows, slots), f32),
            VMEM((slots, slots), bf16),
            VMEM((slots, heads), bf16),
            VMEM(out_weight.shape, bf16),
            VMEM((slots, cols), bf16),
            VMEM((rows, cols), bf16),
            dma((5,)), dma((count,)), dma((count,)), dma((replicas - 1,)), dma((replicas - 1,)),
        ],
        compiler_params=pltpu.CompilerParams(
            collective_id=0, has_side_effects=True, vmem_limit_bytes=58 << 20
        ),
        name="attend",
    )(requests, lengths, routes, queries, keys, values, out_weight, residual)


def layer_kernel(
    part_ref, res_ref, delta_ref, lane_ref, gain_ref, router_ref, gate_hbm, up_hbm, down_hbm,
    out_ref,
    stream, mixed, normed, hidden, combine, packed, w_gate, w_up, w_down,
    slots_c, slots_y, slots_x, sums_y, sums_x, late_y, late_x, local, send, recv,
):
    seq, ten = Ring("seq"), Ring("tensor")
    rows, cols = res_ref.shape
    features = stream.shape[1]
    half, quarter = cols // 2, cols // 4
    loads = [
        pltpu.make_async_copy(src, dst, local.at[i])
        for i, (src, dst) in enumerate(((gate_hbm, w_gate), (up_hbm, w_up), (down_hbm, w_down)))
    ]
    for load in loads:
        load.start()
    greet([seq.next, seq.prev, ten.next, ten.prev])
    c = Copies(send, recv)

    def both(ref, ring):
        return c.start(ref, ref, ring.next), c.start(ref, ref, ring.prev)

    def hop(ref, where):
        return c.start(ref, ref, where)

    summed = RingSum(
        c, ten, lambda k, h: part_ref.at[span(ten.at(k), rows), pl.ds(h * half, half)], slots_c
    )
    summed.raw()
    summed.middle()

    def tile(t, s, h, q=None):
        width, start = (half, h * half) if q is None else (quarter, h * half + q * quarter)
        return stream.at[span(t, rows), pl.ds(pl.multiple_of(s * cols + start, width), width)]

    def where_of(h, step):
        return (ten.me, seq.at(step)) if h == 0 else (ten.at(step), seq.me)

    firsts, seconds = ((0, seq), (1, ten)), ((0, ten), (1, seq))
    near, wide, far, last = {}, {}, {}, []
    for h, ring in firsts:
        tile(ten.me, seq.me, h)[...] = (
            res_ref[:, h * half:(h + 1) * half].astype(f32) + summed.total(h)
        ).astype(bf16)
        near[h] = both(tile(ten.me, seq.me, h), ring)
    for h, other in seconds:
        wide[h] = [both(tile(ten.me, seq.me, h), other)]
    for h, ring in firsts:
        near[h][0].wait_recv()
        far[h] = [hop(tile(*where_of(h, 3), h, 0), ring.next)]
        near[h][1].wait_recv()
        far[h].append(hop(tile(*where_of(h, 1), h, 1), ring.prev))
    for step in (3, 1):
        for h, other in seconds:
            wide[h].append(both(tile(*where_of(h, step), h), other))
    for h, other in seconds:
        far[h][0].wait_recv()
        far[h][1].wait_recv()
        wide[h].append(both(tile(*where_of(h, 2), h), other))
    for i, step in enumerate((0, 3, 1, 2)):
        for h, other in seconds:
            t, s = where_of(h, step)
            across = (lambda k: (other.at(k), s)) if h == 0 else (lambda k: (t, other.at(k)))
            wide[h][i][0].wait_recv()
            last.append(hop(tile(*across(3), h, 0), other.next))
            wide[h][i][1].wait_recv()
            last.append(hop(tile(*across(1), h, 1), other.prev))
    for copy in last:
        copy.wait_recv()

    order = (2, 1, 3, 0)
    place = {step: i for i, step in enumerate(order)}
    both_rows = 2 * rows

    def norm(i):
        base = seq.at(order[i]) * rows

        @pl.loop(0, rows // 16)
        def _(j):
            wide = stream[pl.ds(pl.multiple_of(base + j * 16, 16), 16), :].astype(f32)
            mean = jnp.sum(wide * wide, axis=1, keepdims=True) / features
            normed[pl.ds(pl.multiple_of(i * rows + j * 16, 16), 16), :] = (
                wide * lax.rsqrt(mean + epsilon) * gain_ref[...]
            ).astype(bf16)

        at = pl.ds(i * rows, rows)
        logits = dot(normed[at, :], router_ref[...], TURNED)
        delta = delta_ref[span(seq.at(order[i]), rows), 0:logits.shape[1]]
        side = delta[:, 0:1]
        gap = jnp.sum(delta * logits, axis=1, keepdims=True) * side
        combine[at, :] = jnp.broadcast_to(
            jnp.where(side == 0.0, 0.0, jax.nn.sigmoid(gap)), (rows, combine.shape[1])
        )

    def gate(j):
        at = pl.ds(j * both_rows, both_rows)
        value = dot(normed[at, :], w_gate[...], TURNED)
        hidden[...] = value / (1.0 + jnp.exp(-value)) * combine[at, 0:1]

    def upward(j):
        at = pl.ds(j * both_rows, both_rows)
        hidden[...] = hidden[...] * dot(normed[at, :], w_up[...], TURNED)

    def down(j, first, count):
        at = pl.ds(j * both_rows, both_rows)

        @pl.loop(first, first + count)
        def _(n):
            across = span(n, 512)
            mixed[at, across] = dot(hidden[...].astype(bf16), w_down[:, across], PLAIN).astype(bf16)

    widths = (slots_y.shape[-1], slots_x.shape[-1])
    starts = (0, 2 * widths[0])

    def term(i, col, h, q):
        at = pl.multiple_of(col * cols + starts[h] + q * widths[h], 128)
        return mixed.at[pl.ds(i * rows, rows), pl.ds(at, widths[h])]

    y = [
        RingSum(c, ten, lambda k, q, i=i: term(i, ten.at(k), 0, q), slots_y.at[i])
        for i in range(RING)
    ]
    x = [
        RingSum(c, seq, lambda k, q, i=i: term(place[k], ten.at(order[i]), 1, q), slots_x.at[i])
        for i in range(RING)
    ]
    final = [
        RingSum(c, ring, lambda k, q, h=h, sums=sums: sums.at[place[k], :, pl.ds(q * widths[h], widths[h])], late)
        for h, ring, sums, late in ((0, seq, sums_y, late_y), (1, ten, sums_x, late_x))
    ]

    def settle(h, i):
        source, sums = (y, sums_y) if h == 0 else (x, sums_x)
        for q in range(2):
            sums[i, :, q * widths[h]:(q + 1) * widths[h]] = source[i].total(q).astype(bf16)

    blocks = features // 512
    norm(0)
    norm(1)
    for load in loads:
        load.wait()
    gate(0)
    upward(0)
    down(0, 0, blocks)
    y[0].raw()
    y[1].raw()
    norm(2)
    norm(3)
    y[0].middle()
    gate(1)
    y[1].middle()
    upward(1)
    settle(0, 0)
    final[0].far()
    down(1, 0, blocks)
    y[2].raw()
    x[0].raw()
    y[3].raw()
    x[1].raw()
    settle(0, 1)
    final[0].ahead()
    x[0].middle()
    x[2].raw()
    y[2].middle()
    x[1].middle()
    x[3].raw()
    y[3].middle()
    x[2].middle()
    settle(1, 0)
    final[1].far()
    settle(0, 2)
    final[0].behind()
    final[0].middle()
    x[3].middle()
    settle(1, 1)
    final[1].ahead()
    settle(1, 2)
    final[1].behind()
    final[1].middle()
    settle(0, 3)
    settle(1, 3)
    sent, passed = [], []
    for h in range(2):
        for q in range(2):
            at = starts[h] + q * widths[h]
            own = stream[span(seq.me, rows), pl.ds(pl.multiple_of(ten.me * cols + at, 128), widths[h])]
            packed[span(seq.me, rows), at:at + widths[h]] = (
                own.astype(f32) + final[h].total(q)
            ).astype(bf16)
        sent.append(both(packed.at[span(seq.me, rows), pl.ds(starts[h], 2 * widths[h])], seq))
    for h in range(2):
        sent[h][0].wait_recv()
        passed.append(hop(packed.at[span(seq.at(3), rows), pl.ds(starts[h], widths[h])], seq.next))
        sent[h][1].wait_recv()
        passed.append(hop(packed.at[span(seq.at(1), rows), pl.ds(starts[h] + widths[h], widths[h])], seq.prev))
    for copy in passed:
        copy.wait_recv()
    query = lax.broadcasted_iota(jnp.int32, (out_ref.shape[0], 1), 0) + seq.me * out_ref.shape[0]
    spread = jnp.where(lane_ref[0:1, :] == query, 1.0, 0.0).astype(bf16)
    out_ref[...] = dot(spread, packed[...], PLAIN).astype(bf16)
    c.drain()


def packed_layer(slots, part, own, delta, lane, gain, router, w_gate, w_up, w_down):
    size, cols = part.shape
    features = gain.shape[1]
    units = w_gate.shape[0]
    rows = size // RING
    wide, slim = 3 * cols // 8, cols // 8
    count = 6 + 40 + 60 + 8
    vmem = pl.BlockSpec(memory_space=VMEM)
    hbm = pl.BlockSpec(memory_space=pltpu.HBM)
    dma = pltpu.SemaphoreType.DMA
    return pl.pallas_call(
        layer_kernel,
        out_shape=jax.ShapeDtypeStruct((slots // RING, cols), bf16),
        in_specs=[vmem] * 6 + [hbm] * 3,
        out_specs=vmem,
        scratch_shapes=[
            VMEM((size, features), bf16),
            VMEM((size, features), bf16),
            VMEM((size, features), bf16),
            VMEM((size // 2, units), f32),
            VMEM((size, 128), f32),
            VMEM((size, cols), bf16),
            VMEM((units, features), bf16),
            VMEM((units, features), bf16),
            VMEM((units, features), bf16),
            VMEM((8, rows, cols // 2), bf16),
            VMEM((RING, 8, rows, wide), bf16),
            VMEM((RING, 8, rows, slim), bf16),
            VMEM((RING, rows, 2 * wide), bf16),
            VMEM((RING, rows, 2 * slim), bf16),
            VMEM((8, rows, wide), bf16),
            VMEM((8, rows, slim), bf16),
            dma((3,)), dma((count,)), dma((count,)),
        ],
        compiler_params=pltpu.CompilerParams(
            collective_id=1, has_side_effects=True, vmem_limit_bytes=56 << 20
        ),
        name="layer",
    )(part, own, delta, lane, gain, router, w_gate, w_up, w_down)


def shards(
    residual, queries, attn_keys, attn_values, lengths, requests, routes,
    out_weight, norm_gain, router, w_gate, w_up, w_down,
):
    part, own, delta, lane, most = attend(
        lax.axis_size("replica"), requests, lengths, routes[0].T,
        queries[0], attn_keys[0], attn_values[0], out_weight, residual[0],
    )
    slots, cols = part.shape
    size = min(WINDOW, slots)
    place = jnp.arange(size, dtype=jnp.int32)[None, :]

    def window(i, out):
        start = jnp.minimum(i * size, slots - size)
        own_start = start + lax.axis_index("tensor") * (size // RING)
        fresh = place + start >= i * size
        lanes = jnp.where(fresh, lax.dynamic_slice(lane, (0, start), (lane.shape[0], size)), -1)
        return out + packed_layer(
            slots,
            lax.dynamic_slice(part, (start, 0), (size, cols)),
            lax.dynamic_slice(own, (own_start, 0), (size // RING, cols)),
            lax.dynamic_slice(delta, (start, 0), (size, delta.shape[1])),
            lanes, norm_gain[None], router.T, w_gate[0], w_up[0], w_down[0],
        )

    out = lax.fori_loop(
        0, lax.div(most[0, 0] + (size - 1), size), window, jnp.zeros((slots // RING, cols), bf16)
    )
    return out[None]


def solution(mesh):
    return jax.shard_map(
        shards,
        mesh=mesh,
        in_specs=(
            P("replica", None, None),
            P("replica", "seq", "tensor"),
            P("replica", "seq", "tensor"),
            P("replica", "seq", "tensor"),
            P("replica", None),
            P("replica", None),
            P("replica", None, None),
            P("tensor", "seq"),
            P(),
            P(),
            P(None, ("seq", "tensor"), None),
            P(None, ("seq", "tensor"), None),
            P(None, ("seq", "tensor"), None),
        ),
        out_specs=P("replica", "seq", "tensor"),
        check_vma=False,
    )
```

```python
import functools
import math

import jax
import jax.numpy as jnp
from jax import lax
from jax.experimental import pallas as pl
from jax.experimental.pallas import tpu as pltpu
from jax.sharding import PartitionSpec as P

HEAD_DIM = 128
RING = 4
MESH = pl.DeviceIdType.MESH
VMEM = pltpu.VMEM
WINDOW = 640

masked_score = -1e30
epsilon = 1e-05
f32 = jnp.float32
bf16 = jnp.bfloat16


class Copies:
    def __init__(self, send, recv):
        self.send, self.recv, self.count = send, recv, 0
        self.made = []

    def start(self, src, dst, where):
        n = self.count
        self.count += 1
        copy = pltpu.make_async_remote_copy(
            src_ref=src,
            dst_ref=dst,
            send_sem=self.send.at[n],
            recv_sem=self.recv.at[n],
            device_id=where,
            device_id_type=MESH,
        )
        copy.start()
        self.made.append(copy)
        return copy

    def drain(self):
        for copy in self.made:
            copy.wait_send()


class Ring:
    def __init__(self, axis):
        self.axis = axis
        self.me = lax.axis_index(axis)
        self.next = {axis: self.at(1)}
        self.prev = {axis: self.at(RING - 1)}

    def at(self, step):
        return lax.rem(self.me + step, RING)


def greet(devices):
    barrier = pltpu.get_barrier_semaphore()
    for device in devices:
        pl.semaphore_signal(barrier, inc=1, device_id=device, device_id_type=MESH)
    pl.semaphore_wait(barrier, len(devices))


def span(index, size):
    return pl.ds(pl.multiple_of(index * size, size), size)


def dot(a, b, contract):
    return lax.dot_general(a, b, (contract, ((), ())), preferred_element_type=f32)


PLAIN = ((1,), (0,))
TURNED = ((1,), (1,))


class RingSum:
    def __init__(self, copies, ring, block, slots):
        self.copies, self.ring, self.block, self.slots = copies, ring, block, slots

    def far(self):
        c, r, s = self.copies, self.ring, self.slots
        self.a = c.start(self.block(2, 0), s.at[0], r.next)
        self.b = c.start(self.block(2, 1), s.at[1], r.prev)

    def ahead(self):
        self.c = self.copies.start(self.block(1, 1), self.slots.at[2], self.ring.next)

    def behind(self):
        self.d = self.copies.start(self.block(3, 0), self.slots.at[3], self.ring.prev)

    def raw(self):
        self.far()
        self.ahead()
        self.behind()

    def middle(self):
        c, r, s = self.copies, self.ring, self.slots
        self.a.wait_recv()
        s[6] = (self.block(1, 0)[...].astype(f32) + s[0].astype(f32)).astype(bf16)
        self.e = c.start(s.at[6], s.at[4], r.next)
        self.b.wait_recv()
        s[7] = (self.block(3, 1)[...].astype(f32) + s[1].astype(f32)).astype(bf16)
        self.f = c.start(s.at[7], s.at[5], r.prev)

    def total(self, half):
        s = self.slots
        if half == 0:
            self.d.wait_recv()
            self.e.wait_recv()
            near, far = s[3], s[4]
        else:
            self.c.wait_recv()
            self.f.wait_recv()
            near, far = s[2], s[5]
        own = self.block(0, half)[...]
        return own.astype(f32) + near.astype(f32) + far.astype(f32)


def attention_kernel(
    replicas, req_ref, len_ref, routes_ref, q_hbm, k_hbm, v_hbm, w_hbm, res_hbm,
    part_ref, own_ref, delta_ref, lane_ref, turns_ref,
    req, every, q_ref, kv, bias, pick, att_ref, w_ref, res_ref, proj,
    local, send, recv, req_send, req_recv,
):
    seq = Ring("seq")
    me = lax.axis_index("replica")
    rows = q_ref.shape[0]
    slots = RING * rows
    wide = k_hbm.shape[1]
    kv_count = wide // HEAD_DIM
    group = q_ref.shape[1] // wide
    cols = w_ref.shape[1]
    loads = [
        pltpu.make_async_copy(src, dst, local.at[i])
        for i, (src, dst) in enumerate((
            (k_hbm, kv.at[seq.me, :, pl.ds(0, wide)]),
            (v_hbm, kv.at[seq.me, :, pl.ds(wide, wide)]),
            (q_hbm, q_ref),
            (res_hbm.at[:, span(seq.me, cols)], res_ref),
            (w_hbm, w_ref),
        ))
    ]
    for load in loads:
        load.start()
    req[...] = jnp.zeros_like(req)
    req[0:1, 0:RING] = req_ref[...].astype(f32)
    others = [{"replica": lax.rem(me + d, replicas)} for d in range(1, replicas)]
    greet([seq.next, seq.prev] + others)
    c = Copies(send, recv)
    loads[0].wait()
    loads[1].wait()
    first = [c.start(kv.at[seq.me], kv.at[seq.me], where) for where in (seq.next, seq.prev)]
    asked = Copies(req_send, req_recv)
    for other in others:
        asked.start(req, every.at[me], other)
    every[me] = req[...]

    for copy in asked.made:
        copy.wait_recv()
    wanted = jnp.max(every[...], axis=1)
    lane = lax.broadcasted_iota(jnp.int32, wanted.shape, 1)
    admitted = jnp.where(lane == 0, wanted, 0.0)
    for b in range(1, RING):
        total = jnp.sum(
            jnp.sum(jnp.where(lane == b - 1, admitted, 0.0), axis=1, keepdims=True), axis=0, keepdims=True
        )
        scaled = wanted * float(replicas * rows // 4)
        share = jnp.floor(scaled / total)
        left = scaled - share * total
        share = jnp.where(left < 0, share - 1, jnp.where(left >= total, share + 1, share))
        admitted = jnp.where(lane == b, jnp.minimum(wanted, jnp.maximum(1.0, share)), admitted)
    most = jnp.max(jnp.sum(admitted, axis=1, keepdims=True), axis=0, keepdims=True)
    turns_ref[0] = lax.div(most[0, 0].astype(jnp.int32) + (WINDOW - 1), WINDOW)
    mine = lax.broadcasted_iota(jnp.int32, wanted.shape, 0) == me
    row = jnp.sum(jnp.where(mine, admitted, 0.0), axis=0, keepdims=True)
    lane_one = lax.broadcasted_iota(jnp.int32, row.shape, 1)
    caps = [jnp.sum(jnp.where(lane_one == b, row, 0.0), axis=1, keepdims=True).astype(jnp.int32) for b in range(RING)]
    prompts = len_ref.shape[1]
    length = len_ref[...].astype(f32)
    lane_len = lax.broadcasted_iota(jnp.int32, length.shape, 1)
    lens = [
        jnp.sum(jnp.where(lane_len == b, length, 0.0), axis=1, keepdims=True).astype(jnp.int32)
        for b in range(prompts)
    ]

    def slot_of(place):
        found = jnp.full(place.shape, -1, jnp.int32)
        start = jnp.zeros((1, 1), jnp.int32)
        for b in range(RING):
            stop = start + caps[b]
            found = jnp.where((place >= start) & (place < stop), place - start + b * rows, found)
            start = stop
        return found

    lane_ref[...] = slot_of(lax.broadcasted_iota(jnp.int32, lane_ref.shape, 1))
    key = lax.broadcasted_iota(jnp.int32, (1, slots), 1)
    live = jnp.zeros((1, slots), jnp.int32)
    for b in range(RING):
        live = jnp.where((key >= b * rows) & (key < b * rows + caps[b]), 1, live)
    query = lax.broadcasted_iota(jnp.int32, (rows, 1), 0) + seq.me * rows
    begin = jnp.zeros((rows, 1), jnp.int32)
    end = jnp.zeros((1, 1), jnp.int32)
    for j in range(prompts):
        end = end + lens[j]
        begin = begin + jnp.where(end <= query, lens[j], 0)
    allowed = (key <= query) & (key >= begin) & ((live == 1) | (key == query))
    bias[...] = jnp.where(allowed, 0.0, masked_score)

    half = rows // 2
    first[0].wait_recv()
    before, after = kv.at[seq.at(3), pl.ds(0, half)], kv.at[seq.at(1), pl.ds(half, half)]
    on = c.start(before, before, seq.next)
    first[1].wait_recv()
    back = c.start(after, after, seq.prev)

    @pl.loop(0, slots // 128)
    def _(i):
        place = lax.broadcasted_iota(jnp.int32, (128, 1), 0) + i * 128
        pick[span(i, 128), :] = jnp.where(slot_of(place) == key, 1.0, 0.0).astype(bf16)

    expert = lax.broadcasted_iota(jnp.int32, (128, slots), 0)
    gap = jnp.where(routes_ref[0:1, :] == expert, 1.0, 0.0) - jnp.where(routes_ref[1:2, :] == expert, 1.0, 0.0)
    delta_ref[...] = dot(pick[...], gap.astype(bf16), TURNED)
    on.wait_recv()
    back.wait_recv()
    loads[2].wait()

    scale = 1.0 / math.sqrt(HEAD_DIM)
    pair = 2 * HEAD_DIM
    pairs = q_ref.shape[1] // pair
    sent = []
    for p in range(pairs):
        g = 2 * p // group
        keys = kv[:, :, g * HEAD_DIM:(g + 1) * HEAD_DIM].reshape(slots, HEAD_DIM)
        values = kv[:, :, wide + g * HEAD_DIM:wide + (g + 1) * HEAD_DIM].reshape(slots, HEAD_DIM)

        @pl.loop(2 * p, 2 * p + 2)
        def _(h):
            at = span(h, HEAD_DIM)
            scores = dot(q_ref[:, at], keys, TURNED) * scale + bias[...]
            highest = jnp.max(scores, axis=1, keepdims=True)
            weights = jnp.exp(scores - highest).astype(bf16)
            norm = jnp.sum(weights.astype(f32), axis=1, keepdims=True)
            att_ref[span(seq.me, rows), at] = (dot(weights, values, PLAIN) / norm).astype(bf16)

        mine = att_ref.at[span(seq.me, rows), pl.ds(p * pair, pair)]
        sent.append((c.start(mine, mine, seq.next), c.start(mine, mine, seq.prev)))

    def project(block, start):
        proj[...] = dot(att_ref[span(block, rows), :], w_ref[...], PLAIN).astype(bf16)

        @pl.loop(0, RING)
        def _(i):
            chosen = dot(pick[span(i, rows), span(block, rows)], proj[...], PLAIN)
            if not start:
                chosen = chosen + part_ref[span(i, rows), :].astype(f32)
            part_ref[span(i, rows), :] = chosen.astype(bf16)

    loads[3].wait()

    @pl.loop(0, RING)
    def _(i):
        own_ref[span(i, rows), :] = dot(pick[span(i, rows), :], res_ref[...], PLAIN).astype(bf16)

    loads[4].wait()
    project(seq.me, True)
    passed = []
    for p in range(pairs):
        sent[p][0].wait_recv()
        there = att_ref.at[span(seq.at(3), rows), pl.ds(p * pair, HEAD_DIM)]
        passed.append(c.start(there, there, seq.next))
        sent[p][1].wait_recv()
        there = att_ref.at[span(seq.at(1), rows), pl.ds(p * pair + HEAD_DIM, HEAD_DIM)]
        passed.append(c.start(there, there, seq.prev))
    project(seq.at(3), False)
    project(seq.at(1), False)
    for copy in passed:
        copy.wait_recv()
    project(seq.at(2), False)
    asked.drain()
    c.drain()


def attend(replicas, requests, lengths, routes, queries, keys, values, out_weight, residual):
    rows, heads = queries.shape
    slots = RING * rows
    cols = out_weight.shape[1]
    count = 4 + 4 * (heads // (2 * HEAD_DIM))
    vmem = pl.BlockSpec(memory_space=VMEM)
    hbm = pl.BlockSpec(memory_space=pltpu.HBM)
    dma = pltpu.SemaphoreType.DMA
    return pl.pallas_call(
        functools.partial(attention_kernel, replicas),
        out_shape=(
            jax.ShapeDtypeStruct((slots, cols), bf16),
            jax.ShapeDtypeStruct((slots, cols), bf16),
            jax.ShapeDtypeStruct((slots, 128), f32),
            jax.ShapeDtypeStruct((8, slots), jnp.int32),
            jax.ShapeDtypeStruct((1,), jnp.int32),
        ),
        in_specs=[vmem] * 3 + [hbm] * 5,
        out_specs=(vmem,) * 4 + (pl.BlockSpec(memory_space=pltpu.SMEM),),
        scratch_shapes=[
            VMEM((8, 128), f32),
            VMEM((replicas, 8, 128), f32),
            VMEM((rows, heads), bf16),
            VMEM((RING, rows, 2 * keys.shape[1]), bf16),
            VMEM((rows, slots), f32),
            VMEM((slots, slots), bf16),
            VMEM((slots, heads), bf16),
            VMEM(out_weight.shape, bf16),
            VMEM((slots, cols), bf16),
            VMEM((rows, cols), bf16),
            dma((5,)), dma((count,)), dma((count,)), dma((replicas - 1,)), dma((replicas - 1,)),
        ],
        compiler_params=pltpu.CompilerParams(
            collective_id=0, has_side_effects=True, vmem_limit_bytes=57 << 20
        ),
        name="attend",
    )(requests, lengths, routes, queries, keys, values, out_weight, residual)


def layer_kernel(
    turn_ref, part_ref, res_ref, delta_ref, lane_ref, before_ref, gain_ref, router_ref,
    gate_hbm, up_hbm, down_hbm,
    out_ref,
    terms, stream, mixed, scaled, squares, hidden, share, units, packed, w_gate, w_up, w_down,
    slots_c, slots_y, slots_x, sums_y, sums_x, late_y, late_x, local, send, recv,
):
    seq, ten = Ring("seq"), Ring("tensor")
    size, cols = terms.shape
    rows = size // RING
    features = stream.shape[1]
    half, quarter = cols // 2, cols // 4
    loads = [
        pltpu.make_async_copy(src, dst, local.at[i])
        for i, (src, dst) in enumerate(((gate_hbm, w_gate), (up_hbm, w_up), (down_hbm, w_down)))
    ]
    for load in loads:
        load.start()
    greet([seq.next, seq.prev, ten.next, ten.prev])
    c = Copies(send, recv)

    def both(ref, ring):
        return c.start(ref, ref, ring.next), c.start(ref, ref, ring.prev)

    def hop(ref, where):
        return c.start(ref, ref, where)

    slots = part_ref.shape[0]
    begins = [min(w * size, slots - size) for w in range(-(-slots // size))]
    turn = jnp.full((1, 1), turn_ref[0], jnp.int32)

    def chosen(read):
        value = read(begins[0]).astype(f32)
        for w, begin in enumerate(begins[1:], 1):
            value = jnp.where(turn == w, read(begin).astype(f32), value)
        return value

    def window(index, begin):
        return pl.ds(pl.multiple_of(begin + index * rows, math.gcd(begin, rows)), rows)

    summed = RingSum(
        c, ten, lambda k, h: terms.at[span(ten.at(k), rows), pl.ds(h * half, half)], slots_c
    )
    for k in range(RING):
        terms[k * rows:(k + 1) * rows, :] = chosen(lambda begin: part_ref[window(k, begin), :]).astype(bf16)
    summed.raw()
    squares[...] = jnp.zeros_like(squares)
    summed.middle()

    def tile(t, s, h, q=None):
        width, start = (half, h * half) if q is None else (quarter, h * half + q * quarter)
        return stream.at[span(t, rows), pl.ds(pl.multiple_of(s * cols + start, width), width)]

    def where_of(h, step):
        return (ten.me, seq.at(step)) if h == 0 else (ten.at(step), seq.me)

    order = (2, 1, 3, 0)
    place = {step: i for i, step in enumerate(order)}
    both_rows = 2 * rows

    def take(t, s, h):
        base = t * rows
        at = pl.ds(pl.multiple_of(s * cols + h * half, half), half)
        gain = gain_ref[:, at]

        @pl.loop(0, rows // 32)
        def _(j):
            here = pl.ds(pl.multiple_of(base + j * 32, 32), 32)
            values = stream[here, at].astype(f32)
            squares[here, :] += jnp.broadcast_to(
                jnp.sum(values * values, axis=1, keepdims=True), (32, squares.shape[1])
            )
            scaled[here, at] = (values * gain).astype(bf16)

    firsts, seconds = ((0, seq), (1, ten)), ((0, ten), (1, seq))
    near, wide, far, last = {}, {}, {}, []
    for h, ring in firsts:
        tile(ten.me, seq.me, h)[...] = (
            chosen(lambda begin: res_ref[window(ten.me, begin), h * half:(h + 1) * half]) + summed.total(h)
        ).astype(bf16)
        near[h] = both(tile(ten.me, seq.me, h), ring)
    for h, other in seconds:
        wide[h] = [both(tile(ten.me, seq.me, h), other)]
    for h in range(2):
        take(ten.me, seq.me, h)
    for h, ring in firsts:
        near[h][0].wait_recv()
        far[h] = [hop(tile(*where_of(h, 3), h, 0), ring.next)]
        near[h][1].wait_recv()
        far[h].append(hop(tile(*where_of(h, 1), h, 1), ring.prev))
    for step in (3, 1):
        for h, other in seconds:
            wide[h].append(both(tile(*where_of(h, step), h), other))
    for step in (3, 1):
        for h in range(2):
            take(*where_of(h, step), h)
    for h, other in seconds:
        far[h][0].wait_recv()
        far[h][1].wait_recv()
        wide[h].append(both(tile(*where_of(h, 2), h), other))
    for h in range(2):
        take(*where_of(h, 2), h)
    for i, step in enumerate((0, 3, 1, 2)):
        arrived = []
        for h, other in seconds:
            t, s = where_of(h, step)
            across = [(other.at(k), s) if h == 0 else (t, other.at(k)) for k in range(RING)]
            wide[h][i][0].wait_recv()
            one = hop(tile(*across[3], h, 0), other.next)
            wide[h][i][1].wait_recv()
            two = hop(tile(*across[1], h, 1), other.prev)
            last.append((one, two, (*across[2], h)))
            arrived += [(*across[3], h), (*across[1], h)]
        for which in arrived:
            take(*which)
    for one, two, which in last:
        one.wait_recv()
        two.wait_recv()
        take(*which)
    for load in loads:
        load.wait()

    def weigh(i):
        here = span(seq.at(order[i]), rows)
        factor = lax.rsqrt(squares[here, 0:1] / features + epsilon)
        logits = dot(scaled[here, :], router_ref[...], TURNED) * factor
        delta = chosen(lambda begin: delta_ref[window(seq.at(order[i]), begin), 0:logits.shape[1]])
        side = delta[:, 0:1]
        gap = jnp.sum(delta * logits, axis=1, keepdims=True) * side
        weight = jnp.where(side == 0.0, 0.0, jax.nn.sigmoid(gap))
        units[0, i * rows:(i + 1) * rows, :] = jnp.broadcast_to(factor, (rows, units.shape[2]))
        units[1, i * rows:(i + 1) * rows, :] = jnp.broadcast_to(weight * factor, (rows, units.shape[2]))

    def pair(j):
        return jnp.concatenate(
            [scaled[span(seq.at(order[i]), rows), :] for i in (2 * j, 2 * j + 1)], axis=0
        )

    def gate(j):
        at = pl.ds(j * both_rows, both_rows)
        value = dot(pair(j), w_gate[...], TURNED) * units[0, at, 0:1]
        hidden[...] = value / (1.0 + jnp.exp(-value)) * units[1, at, 0:1]

    def upward(j):
        value = hidden[...] * dot(pair(j), w_up[...], TURNED)
        share[...] = value.astype(bf16)

    def down(j):
        at = pl.ds(j * both_rows, both_rows)

        @pl.loop(0, features // 1024)
        def _(n):
            across = span(n, 1024)
            mixed[at, across] = dot(share[...], w_down[:, across], PLAIN).astype(bf16)

    widths = (slots_y.shape[-1], slots_x.shape[-1])
    starts = (0, 2 * widths[0])

    def term(i, col, h, q):
        at = pl.multiple_of(col * cols + starts[h] + q * widths[h], 128)
        return mixed.at[pl.ds(i * rows, rows), pl.ds(at, widths[h])]

    y = [
        RingSum(c, ten, lambda k, q, i=i: term(i, ten.at(k), 0, q), slots_y.at[i])
        for i in range(RING)
    ]
    x = [
        RingSum(c, seq, lambda k, q, i=i: term(place[k], ten.at(order[i]), 1, q), slots_x.at[i])
        for i in range(RING)
    ]
    final = [
        RingSum(c, ring, lambda k, q, h=h, sums=sums: sums.at[place[k], :, pl.ds(q * widths[h], widths[h])], late)
        for h, ring, sums, late in ((0, seq, sums_y, late_y), (1, ten, sums_x, late_x))
    ]

    def settle(h, i):
        source, sums = (y, sums_y) if h == 0 else (x, sums_x)
        for q in range(2):
            sums[i, :, q * widths[h]:(q + 1) * widths[h]] = source[i].total(q).astype(bf16)

    weigh(0)
    weigh(1)
    gate(0)
    upward(0)
    down(0)
    y[0].raw()
    y[1].raw()
    weigh(2)
    weigh(3)
    y[0].middle()
    gate(1)
    y[1].middle()
    upward(1)
    settle(0, 0)
    final[0].far()
    down(1)
    y[2].raw()
    x[0].raw()
    y[3].raw()
    x[1].raw()
    settle(0, 1)
    final[0].ahead()
    x[0].middle()
    x[2].raw()
    y[2].middle()
    x[1].middle()
    x[3].raw()
    y[3].middle()
    x[2].middle()
    settle(1, 0)
    final[1].far()
    settle(0, 2)
    final[0].behind()
    final[0].middle()
    x[3].middle()
    settle(1, 1)
    final[1].ahead()
    settle(1, 2)
    final[1].behind()
    final[1].middle()
    settle(0, 3)
    settle(1, 3)
    sent, passed = [], []
    for h in range(2):
        for q in range(2):
            at = starts[h] + q * widths[h]
            own = stream[span(seq.me, rows), pl.ds(pl.multiple_of(ten.me * cols + at, 128), widths[h])]
            packed[span(seq.me, rows), at:at + widths[h]] = (
                own.astype(f32) + final[h].total(q)
            ).astype(bf16)
        sent.append(both(packed.at[span(seq.me, rows), pl.ds(starts[h], 2 * widths[h])], seq))
    for h in range(2):
        sent[h][0].wait_recv()
        passed.append(hop(packed.at[span(seq.at(3), rows), pl.ds(starts[h], widths[h])], seq.next))
        sent[h][1].wait_recv()
        passed.append(hop(packed.at[span(seq.at(1), rows), pl.ds(starts[h] + widths[h], widths[h])], seq.prev))
    for copy in passed:
        copy.wait_recv()
    query = lax.broadcasted_iota(jnp.int32, (out_ref.shape[0], 1), 0) + seq.me * out_ref.shape[0]
    slot = lane_ref[0:1, 0:size]
    for w, begin in enumerate(begins[1:], 1):
        row = lax.broadcasted_iota(jnp.int32, slot.shape, 1) + begin
        later = jnp.where(row >= w * size, lane_ref[0:1, begin:begin + size], -1)
        slot = jnp.where(turn == w, later, slot)
    spread = jnp.where(slot == query, 1.0, 0.0).astype(bf16)
    out_ref[...] = (before_ref[...].astype(f32) + dot(spread, packed[...], PLAIN)).astype(bf16)
    c.drain()


def packed_layer(size, turn, part, own, delta, lane, before, gain, router, w_gate, w_up, w_down):
    cols = part.shape[1]
    features = gain.shape[1]
    units = w_gate.shape[0]
    rows = size // RING
    wide, slim = 3 * cols // 8, cols // 8
    count = 6 + 40 + 60 + 8
    vmem = pl.BlockSpec(memory_space=VMEM)
    hbm = pl.BlockSpec(memory_space=pltpu.HBM)
    dma = pltpu.SemaphoreType.DMA
    return pl.pallas_call(
        layer_kernel,
        out_shape=jax.ShapeDtypeStruct(before.shape, bf16),
        in_specs=[pl.BlockSpec(memory_space=pltpu.SMEM)] + [vmem] * 7 + [hbm] * 3,
        out_specs=vmem,
        scratch_shapes=[
            VMEM((size, cols), bf16),
            VMEM((size, features), bf16),
            VMEM((size, features), bf16),
            VMEM((size, features), bf16),
            VMEM((size, 128), f32),
            VMEM((size // 2, units), f32),
            VMEM((size // 2, units), bf16),
            VMEM((2, size, 128), f32),
            VMEM((size, cols), bf16),
            VMEM((units, features), bf16),
            VMEM((units, features), bf16),
            VMEM((units, features), bf16),
            VMEM((8, rows, cols // 2), bf16),
            VMEM((RING, 8, rows, wide), bf16),
            VMEM((RING, 8, rows, slim), bf16),
            VMEM((RING, rows, 2 * wide), bf16),
            VMEM((RING, rows, 2 * slim), bf16),
            VMEM((8, rows, wide), bf16),
            VMEM((8, rows, slim), bf16),
            dma((3,)), dma((count,)), dma((count,)),
        ],
        compiler_params=pltpu.CompilerParams(
            collective_id=1, has_side_effects=True, vmem_limit_bytes=56 << 20
        ),
        name="layer",
    )(turn, part, own, delta, lane, before, gain, router, w_gate, w_up, w_down)


def shards(
    residual, queries, attn_keys, attn_values, lengths, requests, routes,
    out_weight, norm_gain, router, w_gate, w_up, w_down,
):
    part, own, delta, lane, turns = attend(
        lax.axis_size("replica"), requests, lengths, routes[0].T,
        queries[0], attn_keys[0], attn_values[0], out_weight, residual[0],
    )
    slots, cols = part.shape

    def window(turn, out):
        return packed_layer(
            min(WINDOW, slots), turn[None], part, own, delta, lane, out,
            norm_gain[None], router.T, w_gate[0], w_up[0], w_down[0],
        )

    out = lax.fori_loop(0, turns[0], window, jnp.zeros((slots // RING, cols), bf16))
    return out[None]


def solution(mesh):
    return jax.shard_map(
        shards,
        mesh=mesh,
        in_specs=(
            P("replica", None, None),
            P("replica", "seq", "tensor"),
            P("replica", "seq", "tensor"),
            P("replica", "seq", "tensor"),
            P("replica", None),
            P("replica", None),
            P("replica", None, None),
            P("tensor", "seq"),
            P(),
            P(),
            P(None, ("seq", "tensor"), None),
            P(None, ("seq", "tensor"), None),
            P(None, ("seq", "tensor"), None),
        ),
        out_specs=P("replica", "seq", "tensor"),
        check_vma=False,
    )
```

```python
import functools
import math

import jax
import jax.numpy as jnp
from jax import lax
from jax.experimental import pallas as pl
from jax.experimental.pallas import tpu as pltpu
from jax.sharding import PartitionSpec as P

HEAD_DIM = 128
RING = 4
MESH = pl.DeviceIdType.MESH
VMEM = pltpu.VMEM
WINDOW = 640

masked_score = -1e30
epsilon = 1e-05
f32 = jnp.float32
bf16 = jnp.bfloat16


class Copies:
    def __init__(self, send, recv):
        self.send, self.recv, self.count = send, recv, 0
        self.made = []

    def start(self, src, dst, where):
        n = self.count
        self.count += 1
        copy = pltpu.make_async_remote_copy(
            src_ref=src,
            dst_ref=dst,
            send_sem=self.send.at[n],
            recv_sem=self.recv.at[n],
            device_id=where,
            device_id_type=MESH,
        )
        copy.start()
        self.made.append(copy)
        return copy

    def drain(self):
        for copy in self.made:
            copy.wait_send()


class Ring:
    def __init__(self, axis):
        self.axis = axis
        self.me = lax.axis_index(axis)
        self.next = {axis: self.at(1)}
        self.prev = {axis: self.at(RING - 1)}

    def at(self, step):
        return lax.rem(self.me + step, RING)


def greet(devices):
    barrier = pltpu.get_barrier_semaphore()
    for device in devices:
        pl.semaphore_signal(barrier, inc=1, device_id=device, device_id_type=MESH)
    pl.semaphore_wait(barrier, len(devices))


def span(index, size):
    return pl.ds(pl.multiple_of(index * size, size), size)


def dot(a, b, contract):
    return lax.dot_general(a, b, (contract, ((), ())), preferred_element_type=f32)


PLAIN = ((1,), (0,))
TURNED = ((1,), (1,))


class RingSum:
    def __init__(self, copies, ring, block, slots):
        self.copies, self.ring, self.block, self.slots = copies, ring, block, slots

    def first(self):
        c, r, s = self.copies, self.ring, self.slots
        self.a = c.start(self.block(2, 0), s.at[0], r.next)
        self.behind()

    def second(self):
        c, r, s = self.copies, self.ring, self.slots
        self.b = c.start(self.block(2, 1), s.at[1], r.prev)
        self.ahead()

    def far(self):
        c, r, s = self.copies, self.ring, self.slots
        self.a = c.start(self.block(2, 0), s.at[0], r.next)
        self.b = c.start(self.block(2, 1), s.at[1], r.prev)

    def ahead(self):
        self.c = self.copies.start(self.block(1, 1), self.slots.at[2], self.ring.next)

    def behind(self):
        self.d = self.copies.start(self.block(3, 0), self.slots.at[3], self.ring.prev)

    def raw(self):
        self.far()
        self.ahead()
        self.behind()

    def middle(self):
        c, r, s = self.copies, self.ring, self.slots
        self.a.wait_recv()
        s[6] = (self.block(1, 0)[...].astype(f32) + s[0].astype(f32)).astype(bf16)
        self.e = c.start(s.at[6], s.at[4], r.next)
        self.b.wait_recv()
        s[7] = (self.block(3, 1)[...].astype(f32) + s[1].astype(f32)).astype(bf16)
        self.f = c.start(s.at[7], s.at[5], r.prev)

    def total(self, half):
        s = self.slots
        if half == 0:
            self.d.wait_recv()
            self.e.wait_recv()
            near, far = s[3], s[4]
        else:
            self.c.wait_recv()
            self.f.wait_recv()
            near, far = s[2], s[5]
        own = self.block(0, half)[...]
        return own.astype(f32) + near.astype(f32) + far.astype(f32)


def attention_kernel(
    replicas, req_ref, len_ref, routes_ref, q_hbm, k_hbm, v_hbm, w_hbm, res_hbm,
    part_ref, own_ref, delta_ref, lane_ref, turns_ref,
    req, every, q_ref, kv, bias, pick, att_ref, w_ref, res_ref, proj,
    local, send, recv, req_send, req_recv,
):
    seq = Ring("seq")
    me = lax.axis_index("replica")
    rows = q_ref.shape[0]
    slots = RING * rows
    wide = k_hbm.shape[1]
    kv_count = wide // HEAD_DIM
    group = q_ref.shape[1] // wide
    cols = w_ref.shape[1]
    loads = [
        pltpu.make_async_copy(src, dst, local.at[i])
        for i, (src, dst) in enumerate((
            (k_hbm, kv.at[seq.me, :, pl.ds(0, wide)]),
            (v_hbm, kv.at[seq.me, :, pl.ds(wide, wide)]),
            (q_hbm, q_ref),
            (res_hbm.at[:, span(seq.me, cols)], res_ref),
            (w_hbm, w_ref),
        ))
    ]
    for load in loads:
        load.start()
    req[...] = jnp.zeros_like(req)
    req[0:1, 0:RING] = req_ref[...].astype(f32)
    others = [{"replica": lax.rem(me + d, replicas)} for d in range(1, replicas)]
    greet([seq.next, seq.prev] + others)
    c = Copies(send, recv)
    loads[0].wait()
    loads[1].wait()
    first = [c.start(kv.at[seq.me], kv.at[seq.me], where) for where in (seq.next, seq.prev)]
    asked = Copies(req_send, req_recv)
    for other in others:
        asked.start(req, every.at[me], other)
    every[me] = req[...]

    for copy in asked.made:
        copy.wait_recv()
    wanted = jnp.max(every[...], axis=1)
    lane = lax.broadcasted_iota(jnp.int32, wanted.shape, 1)
    admitted = jnp.where(lane == 0, wanted, 0.0)
    for b in range(1, RING):
        total = jnp.sum(
            jnp.sum(jnp.where(lane == b - 1, admitted, 0.0), axis=1, keepdims=True), axis=0, keepdims=True
        )
        scaled = wanted * float(replicas * rows // 4)
        share = jnp.floor(scaled / total)
        left = scaled - share * total
        share = jnp.where(left < 0, share - 1, jnp.where(left >= total, share + 1, share))
        admitted = jnp.where(lane == b, jnp.minimum(wanted, jnp.maximum(1.0, share)), admitted)
    most = jnp.max(jnp.sum(admitted, axis=1, keepdims=True), axis=0, keepdims=True)
    turns_ref[0] = lax.div(most[0, 0].astype(jnp.int32) + (WINDOW - 1), WINDOW)
    mine = lax.broadcasted_iota(jnp.int32, wanted.shape, 0) == me
    row = jnp.sum(jnp.where(mine, admitted, 0.0), axis=0, keepdims=True)
    lane_one = lax.broadcasted_iota(jnp.int32, row.shape, 1)
    caps = [jnp.sum(jnp.where(lane_one == b, row, 0.0), axis=1, keepdims=True).astype(jnp.int32) for b in range(RING)]
    prompts = len_ref.shape[1]
    length = len_ref[...].astype(f32)
    lane_len = lax.broadcasted_iota(jnp.int32, length.shape, 1)
    lens = [
        jnp.sum(jnp.where(lane_len == b, length, 0.0), axis=1, keepdims=True).astype(jnp.int32)
        for b in range(prompts)
    ]

    def slot_of(place):
        found = jnp.full(place.shape, -1, jnp.int32)
        start = jnp.zeros((1, 1), jnp.int32)
        for b in range(RING):
            stop = start + caps[b]
            found = jnp.where((place >= start) & (place < stop), place - start + b * rows, found)
            start = stop
        return found

    lane_ref[...] = slot_of(lax.broadcasted_iota(jnp.int32, lane_ref.shape, 1))
    key = lax.broadcasted_iota(jnp.int32, (1, slots), 1)
    live = jnp.zeros((1, slots), jnp.int32)
    for b in range(RING):
        live = jnp.where((key >= b * rows) & (key < b * rows + caps[b]), 1, live)
    query = lax.broadcasted_iota(jnp.int32, (rows, 1), 0) + seq.me * rows
    begin = jnp.zeros((rows, 1), jnp.int32)
    end = jnp.zeros((1, 1), jnp.int32)
    for j in range(prompts):
        end = end + lens[j]
        begin = begin + jnp.where(end <= query, lens[j], 0)
    allowed = (key <= query) & (key >= begin) & ((live == 1) | (key == query))
    bias[...] = jnp.where(allowed, 0.0, masked_score)

    half = rows // 2
    first[0].wait_recv()
    before, after = kv.at[seq.at(3), pl.ds(0, half)], kv.at[seq.at(1), pl.ds(half, half)]
    on = c.start(before, before, seq.next)
    first[1].wait_recv()
    back = c.start(after, after, seq.prev)

    @pl.loop(0, slots // 128)
    def _(i):
        place = lax.broadcasted_iota(jnp.int32, (128, 1), 0) + i * 128
        pick[span(i, 128), :] = jnp.where(slot_of(place) == key, 1.0, 0.0).astype(bf16)

    expert = lax.broadcasted_iota(jnp.int32, (128, slots), 0)
    gap = jnp.where(routes_ref[0:1, :] == expert, 1.0, 0.0) - jnp.where(routes_ref[1:2, :] == expert, 1.0, 0.0)
    delta_ref[...] = dot(pick[...], gap.astype(bf16), TURNED)
    on.wait_recv()
    back.wait_recv()
    loads[2].wait()

    scale = 1.0 / math.sqrt(HEAD_DIM)
    pair = 2 * HEAD_DIM
    pairs = q_ref.shape[1] // pair
    sent = []
    for p in range(pairs):
        g = 2 * p // group
        keys = kv[:, :, g * HEAD_DIM:(g + 1) * HEAD_DIM].reshape(slots, HEAD_DIM)
        values = kv[:, :, wide + g * HEAD_DIM:wide + (g + 1) * HEAD_DIM].reshape(slots, HEAD_DIM)

        @pl.loop(2 * p, 2 * p + 2)
        def _(h):
            at = span(h, HEAD_DIM)
            scores = dot(q_ref[:, at], keys, TURNED) * scale + bias[...]
            highest = jnp.max(scores, axis=1, keepdims=True)
            weights = jnp.exp(scores - highest).astype(bf16)
            norm = jnp.sum(weights.astype(f32), axis=1, keepdims=True)
            att_ref[span(seq.me, rows), at] = (dot(weights, values, PLAIN) / norm).astype(bf16)

        mine = att_ref.at[span(seq.me, rows), pl.ds(p * pair, pair)]
        sent.append((c.start(mine, mine, seq.next), c.start(mine, mine, seq.prev)))

    def project(block, start):
        proj[...] = dot(att_ref[span(block, rows), :], w_ref[...], PLAIN).astype(bf16)

        @pl.loop(0, RING)
        def _(i):
            chosen = dot(pick[span(i, rows), span(block, rows)], proj[...], PLAIN)
            if not start:
                chosen = chosen + part_ref[span(i, rows), :].astype(f32)
            part_ref[span(i, rows), :] = chosen.astype(bf16)

    loads[3].wait()

    @pl.loop(0, RING)
    def _(i):
        own_ref[span(i, rows), :] = dot(pick[span(i, rows), :], res_ref[...], PLAIN).astype(bf16)

    loads[4].wait()
    project(seq.me, True)
    passed = []
    for p in range(pairs):
        sent[p][0].wait_recv()
        there = att_ref.at[span(seq.at(3), rows), pl.ds(p * pair, HEAD_DIM)]
        passed.append(c.start(there, there, seq.next))
        sent[p][1].wait_recv()
        there = att_ref.at[span(seq.at(1), rows), pl.ds(p * pair + HEAD_DIM, HEAD_DIM)]
        passed.append(c.start(there, there, seq.prev))
    project(seq.at(3), False)
    project(seq.at(1), False)
    for copy in passed:
        copy.wait_recv()
    project(seq.at(2), False)
    asked.drain()
    c.drain()


def attend(replicas, requests, lengths, routes, queries, keys, values, out_weight, residual):
    rows, heads = queries.shape
    slots = RING * rows
    cols = out_weight.shape[1]
    count = 4 + 4 * (heads // (2 * HEAD_DIM))
    vmem = pl.BlockSpec(memory_space=VMEM)
    hbm = pl.BlockSpec(memory_space=pltpu.HBM)
    dma = pltpu.SemaphoreType.DMA
    return pl.pallas_call(
        functools.partial(attention_kernel, replicas),
        out_shape=(
            jax.ShapeDtypeStruct((slots, cols), bf16),
            jax.ShapeDtypeStruct((slots, cols), bf16),
            jax.ShapeDtypeStruct((slots, 128), f32),
            jax.ShapeDtypeStruct((8, slots), jnp.int32),
            jax.ShapeDtypeStruct((1,), jnp.int32),
        ),
        in_specs=[vmem] * 3 + [hbm] * 5,
        out_specs=(vmem,) * 4 + (pl.BlockSpec(memory_space=pltpu.SMEM),),
        scratch_shapes=[
            VMEM((8, 128), f32),
            VMEM((replicas, 8, 128), f32),
            VMEM((rows, heads), bf16),
            VMEM((RING, rows, 2 * keys.shape[1]), bf16),
            VMEM((rows, slots), f32),
            VMEM((slots, slots), bf16),
            VMEM((slots, heads), bf16),
            VMEM(out_weight.shape, bf16),
            VMEM((slots, cols), bf16),
            VMEM((rows, cols), bf16),
            dma((5,)), dma((count,)), dma((count,)), dma((replicas - 1,)), dma((replicas - 1,)),
        ],
        compiler_params=pltpu.CompilerParams(
            collective_id=0, has_side_effects=True, vmem_limit_bytes=57 << 20
        ),
        name="attend",
    )(requests, lengths, routes, queries, keys, values, out_weight, residual)


def layer_kernel(
    turn_ref, part_ref, res_ref, delta_ref, lane_ref, before_ref, gain_ref, router_ref,
    gate_hbm, up_hbm, down_hbm,
    out_ref,
    terms, stream, mixed, scaled, squares, hidden, share, units, packed, w_gate, w_up, w_down,
    slots_c, slots_y, slots_e, slots_x, sums_x, late_x, spread, laid, base, tail, local, send, recv,
):
    seq, ten = Ring("seq"), Ring("tensor")
    size, cols = terms.shape
    rows = size // RING
    features = stream.shape[1]
    half, quarter = cols // 2, cols // 4
    loads = [
        pltpu.make_async_copy(src, dst, local.at[i])
        for i, (src, dst) in enumerate(((gate_hbm, w_gate), (up_hbm, w_up), (down_hbm, w_down)))
    ]
    for load in loads:
        load.start()
    greet([seq.next, seq.prev, ten.next, ten.prev])
    c = Copies(send, recv)

    def both(ref, ring):
        return c.start(ref, ref, ring.next), c.start(ref, ref, ring.prev)

    def hop(ref, where):
        return c.start(ref, ref, where)

    slots = part_ref.shape[0]
    begins = [min(w * size, slots - size) for w in range(-(-slots // size))]
    turn = jnp.full((1, 1), turn_ref[0], jnp.int32)

    def chosen(read):
        value = read(begins[0]).astype(f32)
        for w, begin in enumerate(begins[1:], 1):
            value = jnp.where(turn == w, read(begin).astype(f32), value)
        return value

    def window(index, begin):
        return pl.ds(pl.multiple_of(begin + index * rows, math.gcd(begin, rows)), rows)

    summed = RingSum(
        c, ten, lambda k, h: terms.at[span(ten.at(k), rows), pl.ds(h * half, half)], slots_c
    )
    for k in range(RING):
        terms[k * rows:(k + 1) * rows, :] = chosen(lambda begin: part_ref[window(k, begin), :]).astype(bf16)
    summed.raw()
    squares[...] = jnp.zeros_like(squares)
    summed.middle()

    def tile(t, s, h, q=None):
        width, start = (half, h * half) if q is None else (quarter, h * half + q * quarter)
        return stream.at[span(t, rows), pl.ds(pl.multiple_of(s * cols + start, width), width)]

    def where_of(h, step):
        return (ten.me, seq.at(step)) if h == 0 else (ten.at(step), seq.me)

    order = (2, 1, 3, 0)
    place = {step: i for i, step in enumerate(order)}
    both_rows = 2 * rows

    def take(t, s, h):
        first = t * rows
        at = pl.ds(pl.multiple_of(s * cols + h * half, half), half)
        gain = gain_ref[:, at]

        @pl.loop(0, rows // 32)
        def _(j):
            here = pl.ds(pl.multiple_of(first + j * 32, 32), 32)
            values = stream[here, at].astype(f32)
            squares[here, :] += jnp.broadcast_to(
                jnp.sum(values * values, axis=1, keepdims=True), (32, squares.shape[1])
            )
            scaled[here, at] = (values * gain).astype(bf16)

    firsts, seconds = ((0, seq), (1, ten)), ((0, ten), (1, seq))
    near, wide, far, last = {}, {}, {}, []
    for h, ring in firsts:
        tile(ten.me, seq.me, h)[...] = (
            chosen(lambda begin: res_ref[window(ten.me, begin), h * half:(h + 1) * half]) + summed.total(h)
        ).astype(bf16)
        near[h] = both(tile(ten.me, seq.me, h), ring)
    for h, other in seconds:
        wide[h] = [both(tile(ten.me, seq.me, h), other)]
    slot = lane_ref[0:1, 0:size]
    for w, begin in enumerate(begins[1:], 1):
        row = lax.broadcasted_iota(jnp.int32, slot.shape, 1) + begin
        later = jnp.where(row >= w * size, lane_ref[0:1, begin:begin + size], -1)
        slot = jnp.where(turn == w, later, slot)

    @pl.loop(0, slots // 128)
    def _(i):
        here = lax.broadcasted_iota(jnp.int32, (128, 1), 0) + i * 128
        spread[span(i, 128), :] = jnp.where(slot == here, 1.0, 0.0).astype(bf16)

    for h in range(2):
        take(ten.me, seq.me, h)
    for h, ring in firsts:
        near[h][0].wait_recv()
        far[h] = [hop(tile(*where_of(h, 3), h, 0), ring.next)]
        near[h][1].wait_recv()
        far[h].append(hop(tile(*where_of(h, 1), h, 1), ring.prev))
    for step in (3, 1):
        for h, other in seconds:
            wide[h].append(both(tile(*where_of(h, step), h), other))
    for step in (3, 1):
        for h in range(2):
            take(*where_of(h, step), h)
    for h, other in seconds:
        far[h][0].wait_recv()
        far[h][1].wait_recv()
        wide[h].append(both(tile(*where_of(h, 2), h), other))
    for h in range(2):
        take(*where_of(h, 2), h)
    for i, step in enumerate((0, 3, 1, 2)):
        arrived = []
        for h, other in seconds:
            t, s = where_of(h, step)
            across = [(other.at(k), s) if h == 0 else (t, other.at(k)) for k in range(RING)]
            wide[h][i][0].wait_recv()
            one = hop(tile(*across[3], h, 0), other.next)
            wide[h][i][1].wait_recv()
            two = hop(tile(*across[1], h, 1), other.prev)
            last.append((one, two, (*across[2], h)))
            arrived += [(*across[3], h), (*across[1], h)]
        for which in arrived:
            take(*which)
    for one, two, which in last:
        one.wait_recv()
        two.wait_recv()
        take(*which)
    for load in loads:
        load.wait()

    def weigh(i):
        here = pl.ds(i * rows, rows)
        factor = lax.rsqrt(squares[here, 0:1] / features + epsilon)
        logits = dot(scaled[here, :], router_ref[...], TURNED) * factor
        delta = chosen(lambda begin: delta_ref[window(i, begin), 0:logits.shape[1]])
        side = delta[:, 0:1]
        gap = jnp.sum(delta * logits, axis=1, keepdims=True) * side
        weight = jnp.where(side == 0.0, 0.0, jax.nn.sigmoid(gap))
        units[0, here, :] = jnp.broadcast_to(factor, (rows, units.shape[2]))
        units[1, here, :] = jnp.broadcast_to(weight * factor, (rows, units.shape[2]))

    def work(j):
        at = pl.ds(j * both_rows, both_rows)
        value = dot(scaled[at, :], w_gate[...], TURNED) * units[0, at, 0:1]
        hidden[...] = value / (1.0 + jnp.exp(-value)) * units[1, at, 0:1]
        share[at, :] = (hidden[...] * dot(scaled[at, :], w_up[...], TURNED)).astype(bf16)

    def down(j, at):
        @pl.loop(0, RING)
        def _(n):
            across = pl.ds(pl.multiple_of(n * cols + j * half, half), half)
            mixed[at, across] = dot(share[at, :], w_down[:, across], PLAIN).astype(bf16)

    def share_of(col, start, width):
        return pl.ds(pl.multiple_of(col * cols + start, 128), width)

    slim = tail.shape[1]
    widths = (quarter, quarter, half - slim)
    y = [
        RingSum(
            c, ten,
            lambda k, q, j=j: mixed.at[
                pl.ds(q * both_rows, both_rows), share_of(ten.at(k), j * quarter, widths[j])
            ],
            slots_y.at[j, :, :, pl.ds(0, widths[j])],
        )
        for j in range(3)
    ]
    part_rows = out_ref.shape[0] // 2
    e = [
        RingSum(
            c, seq,
            lambda k, q, j=j: laid.at[
                j, pl.ds(pl.multiple_of(seq.at(k) * (2 * part_rows) + q * part_rows, part_rows), part_rows),
                pl.ds(0, widths[j]),
            ],
            slots_e.at[j, :, :, pl.ds(0, widths[j])],
        )
        for j in range(3)
    ]

    def lay(j):
        for q in range(2):
            packed[q * both_rows:(q + 1) * both_rows, 0:widths[j]] = y[j].total(q).astype(bf16)

        @pl.loop(0, RING)
        def _(i):
            laid[j, span(i, 2 * part_rows), 0:widths[j]] = dot(
                spread[span(i, 2 * part_rows), :], packed[:, 0:widths[j]], PLAIN
            ).astype(bf16)

        e[j].raw()

    def write(j):
        at = slice(j * quarter, j * quarter + widths[j])
        for q in range(2):
            here = slice(q * part_rows, (q + 1) * part_rows)
            out_ref[here, at] = (base[here, at] + e[j].total(q)).astype(bf16)

    few = rows // 2

    def half_of(index, q):
        return pl.ds(pl.multiple_of(index * rows + q * few, few), few)

    x = [
        RingSum(
            c, seq,
            lambda k, q, i=i: mixed.at[half_of(seq.at(k), q), share_of(ten.at(order[i]), cols - slim, slim)],
            slots_x.at[i],
        )
        for i in range(RING)
    ]
    final = RingSum(c, ten, lambda k, q: sums_x.at[place[k], pl.ds(q * few, few)], late_x)

    def settle(i):
        for q in range(2):
            sums_x[i, q * few:(q + 1) * few, :] = x[i].total(q).astype(bf16)

    above, below = pl.ds(0, both_rows), pl.ds(both_rows, both_rows)
    weigh(0)
    weigh(1)
    work(0)
    down(0, above)
    y[0].first()
    y[1].first()
    weigh(2)
    weigh(3)
    work(1)
    down(1, pl.ds(0, size))
    x[0].raw()
    x[1].raw()
    down(0, below)
    y[0].second()
    y[1].second()
    y[0].middle()
    y[2].raw()
    own_rows = spread[span(seq.me, 2 * part_rows), :]
    base[...] = before_ref[...].astype(f32) + dot(
        own_rows, stream[:, pl.ds(pl.multiple_of(ten.me * cols, cols), cols)], PLAIN
    )
    x[0].middle()
    x[2].raw()
    y[1].middle()
    x[1].middle()
    x[3].raw()
    lay(0)
    x[2].middle()
    y[2].middle()
    x[3].middle()
    settle(0)
    final.far()
    e[0].middle()
    lay(1)
    settle(1)
    final.ahead()
    settle(2)
    final.behind()
    final.middle()
    e[1].middle()
    lay(2)
    settle(3)
    for q in range(2):
        tail[half_of(seq.me, q), :] = final.total(q).astype(bf16)
    mine = tail.at[span(seq.me, rows), :]
    sent = both(mine, seq)
    e[2].middle()
    write(0)
    sent[0].wait_recv()
    passed = [hop(tail.at[half_of(seq.at(3), 0)], seq.next)]
    sent[1].wait_recv()
    passed.append(hop(tail.at[half_of(seq.at(1), 1)], seq.prev))
    write(1)
    for copy in passed:
        copy.wait_recv()
    out_ref[:, cols - slim:] = (
        base[:, cols - slim:] + dot(spread[span(seq.me, 2 * part_rows), :], tail[...], PLAIN)
    ).astype(bf16)
    write(2)
    c.drain()


def packed_layer(size, turn, part, own, delta, lane, before, gain, router, w_gate, w_up, w_down):
    cols = part.shape[1]
    features = gain.shape[1]
    units = w_gate.shape[0]
    rows = size // RING
    slots = part.shape[0]
    quarter, slim = cols // 4, 3 * cols // 8
    count = 6 + 40 + 18 + 18 + 24 + 6 + 4
    vmem = pl.BlockSpec(memory_space=VMEM)
    hbm = pl.BlockSpec(memory_space=pltpu.HBM)
    dma = pltpu.SemaphoreType.DMA
    return pl.pallas_call(
        layer_kernel,
        out_shape=jax.ShapeDtypeStruct(before.shape, bf16),
        in_specs=[pl.BlockSpec(memory_space=pltpu.SMEM)] + [vmem] * 7 + [hbm] * 3,
        out_specs=vmem,
        scratch_shapes=[
            VMEM((size, cols), bf16),
            VMEM((size, features), bf16),
            VMEM((size, features), bf16),
            VMEM((size, features), bf16),
            VMEM((size, 128), f32),
            VMEM((size // 2, units), f32),
            VMEM((size, units), bf16),
            VMEM((2, size, 128), f32),
            VMEM((size, quarter), bf16),
            VMEM((units, features), bf16),
            VMEM((units, features), bf16),
            VMEM((units, features), bf16),
            VMEM((8, rows, cols // 2), bf16),
            VMEM((3, 8, size // 2, quarter), bf16),
            VMEM((3, 8, slots // RING // 2, quarter), bf16),
            VMEM((RING, 8, rows // 2, slim), bf16),
            VMEM((RING, rows, slim), bf16),
            VMEM((8, rows // 2, slim), bf16),
            VMEM((slots, size), bf16),
            VMEM((3, slots, quarter), bf16),
            VMEM((slots // RING, cols), f32),
            VMEM((size, slim), bf16),
            dma((3,)), dma((count,)), dma((count,)),
        ],
        compiler_params=pltpu.CompilerParams(
            collective_id=1, has_side_effects=True, vmem_limit_bytes=56 << 20
        ),
        name="layer",
    )(turn, part, own, delta, lane, before, gain, router, w_gate, w_up, w_down)


def shards(
    residual, queries, attn_keys, attn_values, lengths, requests, routes,
    out_weight, norm_gain, router, w_gate, w_up, w_down,
):
    part, own, delta, lane, turns = attend(
        lax.axis_size("replica"), requests, lengths, routes[0].T,
        queries[0], attn_keys[0], attn_values[0], out_weight, residual[0],
    )
    slots, cols = part.shape

    def window(turn, out):
        return packed_layer(
            min(WINDOW, slots), turn[None], part, own, delta, lane, out,
            norm_gain[None], router.T, w_gate[0], w_up[0], w_down[0],
        )

    out = lax.fori_loop(0, turns[0], window, jnp.zeros((slots // RING, cols), bf16))
    return out[None]


def solution(mesh):
    return jax.shard_map(
        shards,
        mesh=mesh,
        in_specs=(
            P("replica", None, None),
            P("replica", "seq", "tensor"),
            P("replica", "seq", "tensor"),
            P("replica", "seq", "tensor"),
            P("replica", None),
            P("replica", None),
            P("replica", None, None),
            P("tensor", "seq"),
            P(),
            P(),
            P(None, ("seq", "tensor"), None),
            P(None, ("seq", "tensor"), None),
            P(None, ("seq", "tensor"), None),
        ),
        out_specs=P("replica", "seq", "tensor"),
        check_vma=False,
    )
```
